16 devices in a mesh: rep: 4 (over y, z, core), dp: 4 (over x).
Axes of the slice: x: 4, y: 2, z: 1, core: 2. Of those that a mesh axis runs over, the one named last changes fastest.
The devices are a block of a 4x4x8 slice.
Arguments:
- x: bfloat16 [16, 4096, 512], P(('rep', 'dp')), parts along dimension 0
- dy: bfloat16 [16, 4096, 512], P(('rep', 'dp')), parts along dimension 0
- w_gate: bfloat16 [2, 512, 1664], replicated
- w_up: bfloat16 [2, 512, 1664], replicated
- w_down: bfloat16 [2, 1664, 512], replicated
- m_w_gate: float32 [2, 512, 1664], replicated
- m_w_up: float32 [2, 512, 1664], replicated
- m_w_down: float32 [2, 1664, 512], replicated
- v_w_gate: float32 [2, 512, 1664], replicated
- v_w_up: float32 [2, 512, 1664], replicated
- v_w_down: float32 [2, 1664, 512], replicated
Outputs:
- output 1: bfloat16 [8, 512, 1664], P('rep'), parts along dimension 0
- output 2: bfloat16 [8, 512, 1664], P('rep'), parts along dimension 0
- output 3: bfloat16 [8, 1664, 512], P('rep'), parts along dimension 0
- output 4: float32 [8, 512, 1664], P('rep'), parts along dimension 0
- output 5: float32 [8, 512, 1664], P('rep'), parts along dimension 0
- output 6: float32 [8, 1664, 512], P('rep'), parts along dimension 0
- output 7: float32 [8, 512, 1664], P('rep'), parts along dimension 0
- output 8: float32 [8, 512, 1664], P('rep'), parts along dimension 0
- output 9: float32 [8, 1664, 512], P('rep'), parts along dimension 0
There are 4 independent parts. The reference program is written for one: setup_inputs(seed, part) draws one part's arguments, and reference() takes and returns one part's arrays. A program takes and returns all parts, laid end to end along the dimension named above; an argument that names none is the same for every part.
All inputs are finite; a program needn't handle non-finite values.
Results may differ from the reference program's by a relative error of at most 0.02.
Values are sent between devices in bfloat16 or wider.
A program may use at most 768 MiB of HBM per device.

```python
import jax
import jax.numpy as jnp
from jax import lax

SEQUENCES = 4
TOKENS = 4096
D = 512
FF = 1664
LAYERS = 2
NAMES = ("w_gate", "w_up", "w_down")
SHAPES = {"w_gate": (LAYERS, D, FF), "w_up": (LAYERS, D, FF), "w_down": (LAYERS, FF, D)}


def bump(key, n, height):
    away = (jnp.arange(n, dtype=jnp.int32) - jax.random.randint(key, (), 0, n, jnp.int32)) % n
    return jnp.where(away < n // 8, height, 1.0)


def together(key, own, strength):
    shared = jax.random.normal(key, own.shape[1:], jnp.float32)
    return (own + strength * shared) * lax.rsqrt(1 + strength * strength)


def setup_inputs(seed: int = 0, part: int = 0) -> dict:
    kx, kdy, ka, kb, kz, kf, kh, kl, *keys = jax.random.split(jax.random.key(seed), 8 + 3 * len(NAMES))
    kx, kdy, ka, kb = (jax.random.fold_in(k, part) for k in (kx, kdy, ka, kb))
    kw, km, kv = (keys[i::3] for i in range(3))
    shape = (SEQUENCES, TOKENS, D)
    much_x, much_dy = jax.random.uniform(kz, (2,), jnp.float32, 0.0, 1.0)
    loud = 2.0 ** jax.random.uniform(jax.random.fold_in(kz, 1), (), jnp.float32, -1.0, 2.0)
    layers = 2.0 ** jax.random.uniform(kl, (LAYERS, 1, 1), jnp.float32, -1.0, 1.0)
    x = together(ka, jax.random.normal(kx, shape, jnp.float32), much_x) * bump(kf, D, 4.0)
    dy = together(kb, jax.random.normal(kdy, shape, jnp.float32), much_dy)
    drawn = {"x": x.astype(jnp.bfloat16), "dy": (loud * dy * (SEQUENCES * TOKENS) ** -0.5).astype(jnp.bfloat16)}
    for key, name in zip(kw, NAMES, strict=True):
        w = jax.random.normal(key, SHAPES[name], jnp.float32) * SHAPES[name][1] ** -0.5
        drawn[name] = (w * {"w_gate": 1.0, "w_up": bump(kh, FF, 4.0), "w_down": layers}[name]).astype(jnp.bfloat16)
    for key, name in zip(km, NAMES, strict=True):
        drawn[f"m_{name}"] = 0.1 * jax.random.normal(key, SHAPES[name], jnp.float32)
    for key, name in zip(kv, NAMES, strict=True):
        drawn[f"v_{name}"] = jax.random.uniform(key, SHAPES[name], jnp.float32, 0.005, 0.015)
    return drawn


def matmul(a, w):
    return jnp.dot(a, w, preferred_element_type=jnp.float32).astype(jnp.bfloat16)


def normed(h):
    wide = h.astype(jnp.float32)
    scale = lax.rsqrt(jnp.mean(wide**2, -1, keepdims=True) + 1e-6)
    return (wide * scale).astype(jnp.bfloat16)


def layer(h, w):
    a = normed(h)
    gate = jnp.dot(a, w["w_gate"], preferred_element_type=jnp.float32)
    up = jnp.dot(a, w["w_up"], preferred_element_type=jnp.float32)
    return h + matmul((jax.nn.silu(gate) * up).astype(jnp.bfloat16), w["w_down"])


def adamw(w, m, v, g):
    m = 0.9 * m + 0.1 * g
    v = 0.95 * v + 0.05 * g * g
    step = m * lax.rsqrt(v + 1e-8) + 0.1 * w
    return (w - 0.02 * step).astype(jnp.bfloat16), m, v


def stack(weights, h):
    return lax.scan(lambda h, w: (layer(h, w), None), h, weights)[0]


def reference(x, dy, w_gate, w_up, w_down, m_w_gate, m_w_up, m_w_down, v_w_gate, v_w_up, v_w_down):
    weights = dict(zip(NAMES, (w_gate, w_up, w_down), strict=True))

    def take(so_far, sequence):
        h, by_y = sequence
        _, back = jax.vjp(lambda w: stack(w, h), weights)
        return jax.tree.map(lambda total, term: total + term.astype(jnp.float32), so_far, back(by_y)[0]), None

    none_yet = {name: jnp.zeros(w.shape, jnp.float32) for name, w in weights.items()}
    by_weights, _ = lax.scan(take, none_yet, (x, dy))
    gradients = [by_weights[name].astype(jnp.bfloat16).astype(jnp.float32) for name in NAMES]
    new = [
        adamw(w.astype(jnp.float32), m, v, g)
        for w, m, v, g in zip((w_gate, w_up, w_down), (m_w_gate, m_w_up, m_w_down), (v_w_gate, v_w_up, v_w_down), gradients, strict=True)
    ]
    return tuple(one[which] for which in range(3) for one in new)
```

```python
import functools

import jax
import jax.numpy as jnp
from jax import lax
from jax.experimental import pallas as pl
from jax.experimental.pallas import tpu as pltpu
from jax.sharding import PartitionSpec as P

BF16, F32 = jnp.bfloat16, jnp.float32
WIDE = 256
LANES = 128
TILE = 1024
ROWS = 512


def at(index, size):
    if isinstance(index, int):
        return pl.ds(index * size, size)
    return pl.ds(pl.multiple_of(index * size, size), size)


def dot(a, b):
    return jnp.dot(a, b, preferred_element_type=F32)


def dot_t(a, b):
    return lax.dot_general(a, b, (((1,), (1,)), ((), ())), preferred_element_type=F32)


def scale_of(wide):
    return lax.rsqrt(jnp.mean(wide * wide, -1, keepdims=True) + 1e-6)


def normed(h):
    wide = h.astype(F32)
    return (wide * scale_of(wide)).astype(BF16)


def main_kernel(x_hbm, dy_hbm, wg_hbm, wu_hbm, wd_hbm, out_hbm, h_ref, a_ref, at_ref, g_ref, gt_ref, da_ref, wgu_ref, wd_ref, mid_ref, hid_ref, dgu_ref, term_ref, w_sem, x_sem, dy_sem, out_sem):
    tokens, d = h_ref.shape
    layers, ff, _ = wd_ref.shape
    full = ff // WIDE
    widths = [WIDE] * full + ([ff % WIDE] if ff % WIDE else [])

    def weight_copies(layer):
        copies = []
        for k, width in enumerate(widths):
            for source, offset in ((wg_hbm, 0), (wu_hbm, width)):
                copies.append((source.at[layer, :, pl.ds(k * WIDE, width)], wgu_ref.at[layer, :, pl.ds(2 * k * WIDE + offset, width)]))
        copies.append((wd_hbm.at[layer], wd_ref.at[layer]))
        return [pltpu.make_async_copy(source, target, w_sem.at[layer, i]) for i, (source, target) in enumerate(copies)]

    def x_copy(t, target):
        return pltpu.make_async_copy(x_hbm.at[0, at(t, ROWS)], target.at[at(t, ROWS)], x_sem.at[t])

    dy_copy = pltpu.make_async_copy(dy_hbm.at[0], g_ref, dy_sem)
    steps = tokens // ROWS
    for copy in weight_copies(0):
        copy.start()
    for t in range(steps):
        x_copy(t, h_ref).start()
    dy_copy.start()
    for layer in range(1, layers):
        for copy in weight_copies(layer):
            copy.start()
    for copy in weight_copies(0):
        copy.wait()

    def forward(t, carry):
        rows = at(t, ROWS)
        x_copy(t, h_ref).wait()
        x = h_ref[rows, :]
        a = normed(x)
        for k, width in enumerate(widths):
            gu = dot(a, wgu_ref[0, :, pl.ds(2 * k * WIDE, 2 * width)])
            gate, up = gu[:, :width], gu[:, width:]
            mid_ref[:, pl.ds(k * WIDE, width)] = (gate * jax.nn.sigmoid(gate) * up).astype(BF16)
        h = (x.astype(F32) + dot(mid_ref[...], wd_ref[0]).astype(BF16).astype(F32)).astype(BF16)
        h_ref[rows, :] = h
        a = normed(h)
        a_ref[rows, :] = a
        at_ref[:, rows] = a.T
        return carry

    lax.fori_loop(0, steps, forward, 0)
    dy_copy.wait()

    def turn(t, carry):
        rows = at(t, ROWS)
        gt_ref[:, rows] = g_ref[rows, :].T
        return carry

    lax.fori_loop(0, steps, turn, 0)
    for layer in range(1, layers):
        for copy in weight_copies(layer):
            copy.wait()

    def chunk(layer, k, width, first, last):
        gu_cols = pl.ds(pl.multiple_of(k * 2 * WIDE, 2 * WIDE), 2 * width)
        down_rows = pl.ds(pl.multiple_of(k * WIDE, WIDE), width)

        def hidden(t, carry):
            rows = at(t, TILE)
            gu = dot(a_ref[rows, :], wgu_ref[layer, :, gu_cols])
            dh = dot_t(g_ref[rows, :], wd_ref[layer, down_rows, :]).astype(BF16).astype(F32)
            gate, up = gu[:, :width], gu[:, width:]
            s = jax.nn.sigmoid(gate)
            silu = gate * s
            hid_ref[rows, pl.ds(0, width)] = (silu * up).astype(BF16)
            dgu_ref[rows, pl.ds(width, width)] = (dh * silu).astype(BF16)
            dgu_ref[rows, pl.ds(0, width)] = (dh * up * (s + silu * (1.0 - s))).astype(BF16)
            return carry

        lax.fori_loop(0, tokens // TILE, hidden, 0)
        dgu = dot(at_ref[...], dgu_ref[:, pl.ds(0, 2 * width)]).astype(BF16)
        down = dot(gt_ref[...], hid_ref[:, pl.ds(0, width)]).astype(BF16)
        for j in range(width // LANES):
            for i, piece in enumerate((dgu[:, j * LANES : (j + 1) * LANES], dgu[:, width + j * LANES : width + (j + 1) * LANES], down[:, j * LANES : (j + 1) * LANES])):
                term_ref[:, pl.ds(pl.multiple_of(k * 3 * WIDE, 3 * WIDE) + (3 * j + i) * LANES, LANES)] = piece
        if layer:

            def by_a(t, carry):
                rows = at(t, TILE)
                part = dot_t(dgu_ref[rows, pl.ds(0, 2 * width)], wgu_ref[layer, :, gu_cols])
                if first is True:
                    da_ref[rows, :] = part
                else:
                    da_ref[rows, :] += part
                return carry

            lax.fori_loop(0, tokens // TILE, by_a, 0)

    def backward(layer):
        if layer:
            chunk(layer, 0, WIDE, True, False)

            def body(k, carry):
                chunk(layer, k, WIDE, False, False)
                return carry

            lax.fori_loop(1, full, body, 0)
        else:

            def body(k, carry):
                chunk(layer, k, WIDE, False, False)
                return carry

            lax.fori_loop(0, full, body, 0)
        for k in range(full, len(widths)):
            chunk(layer, k, widths[k], False, True)
        copy = pltpu.make_async_copy(term_ref, out_hbm.at[layer], out_sem)
        copy.start()
        copy.wait()

    backward(1)

    for t in range(steps):
        x_copy(t, a_ref).start()

    def between(t, carry):
        rows = at(t, ROWS)
        x_copy(t, a_ref).wait()
        da = da_ref[rows, :].astype(BF16).astype(F32)
        h = h_ref[rows, :].astype(F32)
        r = scale_of(h)
        inner = jnp.mean(da * h, -1, keepdims=True)
        dh = (r * (da - h * (r * r * inner))).astype(BF16).astype(F32)
        g = (g_ref[rows, :].astype(F32) + dh).astype(BF16)
        g_ref[rows, :] = g
        gt_ref[:, rows] = g.T
        a = normed(a_ref[rows, :])
        a_ref[rows, :] = a
        at_ref[:, rows] = a.T
        return carry

    lax.fori_loop(0, steps, between, 0)
    backward(0)


def main_call(x, dy, wg, wu, wd):
    layers, d, ff = wg.shape
    tokens = x.shape[1]
    pieces = 2 * -(-ff // WIDE) + 1
    any_ = pl.BlockSpec(memory_space=pl.ANY)
    return pl.pallas_call(
        main_kernel,
        out_shape=jax.ShapeDtypeStruct((layers, d, 3 * ff), BF16),
        in_specs=[any_] * 5,
        out_specs=any_,
        scratch_shapes=[
            pltpu.VMEM((tokens, d), BF16),
            pltpu.VMEM((tokens, d), BF16),
            pltpu.VMEM((d, tokens), BF16),
            pltpu.VMEM((tokens, d), BF16),
            pltpu.VMEM((d, tokens), BF16),
            pltpu.VMEM((tokens, d), F32),
            pltpu.VMEM((layers, d, 2 * ff), BF16),
            pltpu.VMEM((layers, ff, d), BF16),
            pltpu.VMEM((ROWS, ff), BF16),
            pltpu.VMEM((tokens, WIDE), BF16),
            pltpu.VMEM((tokens, 2 * WIDE), BF16),
            pltpu.VMEM((d, 3 * ff), BF16),
            pltpu.SemaphoreType.DMA((layers, pieces)),
            pltpu.SemaphoreType.DMA((tokens // ROWS,)),
            pltpu.SemaphoreType.DMA,
            pltpu.SemaphoreType.DMA,
        ],
        compiler_params=pltpu.CompilerParams(vmem_limit_bytes=67_000_000),
        name="main",
    )(x, dy, wg, wu, wd)


def adamw(w, m, v, g):
    m = 0.9 * m + 0.1 * g
    v = 0.95 * v + 0.05 * g * g
    step = m * lax.rsqrt(v + 1e-8) + 0.1 * w
    return (w - 0.02 * step).astype(BF16), m, v


def adam_kernel(which, g_ref, *refs):
    ins, outs = refs[:9], refs[-9:]
    ff = ins[0].shape[-1]
    for j in range(ff // LANES):
        cols = pl.ds(j * LANES, LANES)
        for i in range(3):
            g = g_ref[0, :, pl.ds((3 * j + i) * LANES, LANES)].astype(F32)
            index = (0, slice(None), cols)
            if i == 2:
                g, index = g.T, (0, cols, slice(None))
            w, m, v = adamw(ins[i][index].astype(F32), ins[3 + i][index], ins[6 + i][index], g)
            outs[i][index], outs[3 + i][index], outs[6 + i][index] = w, m, v


def adam_call(g, arrays):
    layers, d, ff = arrays[0].shape
    row = pl.BlockSpec((1, LANES, ff), lambda l, r, s: (l, r, 0))
    column = pl.BlockSpec((1, ff, LANES), lambda l, r, s: (l, 0, r))
    specs = [row, row, column] * 3
    return pl.pallas_call(
        adam_kernel,
        grid_spec=pltpu.PrefetchScalarGridSpec(
            num_scalar_prefetch=1,
            grid=(layers, d // LANES),
            in_specs=[pl.BlockSpec((1, LANES, 3 * ff), lambda l, r, s: (l, r, 0))] + specs,
            out_specs=specs,
        ),
        out_shape=[jax.ShapeDtypeStruct(a.shape, a.dtype) for a in arrays],
        compiler_params=pltpu.CompilerParams(vmem_limit_bytes=60_000_000),
        name="adam",
    )(jnp.zeros((1,), jnp.int32), g, *arrays)


def solution(mesh):
    def step(x, dy, *arrays):
        g = main_call(x, dy, *arrays[:3])
        g = lax.psum(g, "dp")
        return tuple(adam_call(g, arrays))

    return jax.shard_map(
        step,
        mesh=mesh,
        in_specs=(P(("rep", "dp"), None, None),) * 2 + (P(None, None, None),) * 9,
        out_specs=(P("rep", None, None),) * 9,
        check_vma=False,
    )
```

```python
import functools

import jax
import jax.numpy as jnp
from jax import lax
from jax.experimental import pallas as pl
from jax.experimental.pallas import tpu as pltpu
from jax.sharding import PartitionSpec as P

BF16, F32 = jnp.bfloat16, jnp.float32
WIDE = 256
LANES = 128
TILE = 1024
ROWS = 512


def at(index, size):
    if isinstance(index, int):
        return pl.ds(index * size, size)
    return pl.ds(pl.multiple_of(index * size, size), size)


def dot(a, b):
    return jnp.dot(a, b, preferred_element_type=F32)


def dot_t(a, b):
    return lax.dot_general(a, b, (((1,), (1,)), ((), ())), preferred_element_type=F32)


def scale_of(wide):
    return lax.rsqrt(jnp.mean(wide * wide, -1, keepdims=True) + 1e-6)


def normed(h):
    wide = h.astype(F32)
    return (wide * scale_of(wide)).astype(BF16)


def main_kernel(
    n, x_hbm, dy_hbm, wg_hbm, wu_hbm, wd_hbm,
    all_hbm, own_hbm,
    h_ref, a_ref, at_ref, g_ref, gt_ref, da_ref, wgu_ref, wd_ref, mid_ref, hid_ref, dgu_ref, term_ref, one_ref, two_ref,
    w_sem, x_sem, dy_sem, one_send, one_recv, two_send, two_recv, near_send, near_recv, far_send, far_recv, keep_sem,
):
    tokens, d = h_ref.shape
    layers, ff, _ = wd_ref.shape
    full = ff // WIDE
    widths = [WIDE] * full + ([ff % WIDE] if ff % WIDE else [])
    share = d // n
    half = share // 2
    me = lax.axis_index("dp")
    right, left, across = (lax.rem(me + i, n) for i in (1, n - 1, 2))
    ways = (right, left)

    barrier = pltpu.get_barrier_semaphore()
    for way in ways:
        pl.semaphore_signal(barrier, inc=1, device_id={"dp": way}, device_id_type=pl.DeviceIdType.MESH)

    def cols_of(k):
        return pl.ds(pl.multiple_of(k * 3 * WIDE, 3 * WIDE), 3 * widths[k] if isinstance(k, int) else 3 * WIDE)

    def rows_of(owner, part=None):
        if part is None:
            return pl.ds(pl.multiple_of(owner * share, share), share)
        return pl.ds(pl.multiple_of(owner * share + part * half, half), half)

    def remote(source, target, send, recv, way):
        return pltpu.make_async_remote_copy(
            src_ref=source, dst_ref=target, send_sem=send, recv_sem=recv, device_id={"dp": ways[way]}, device_id_type=pl.DeviceIdType.MESH
        )

    def one(layer, k, way):
        cols = cols_of(k)
        return remote(term_ref.at[rows_of(across, way), cols], one_ref.at[way, :, cols], one_send.at[layer, k, way], one_recv.at[layer, k, way], way)

    def two(layer, k, way):
        cols = cols_of(k)
        return remote(term_ref.at[rows_of(ways[way]), cols], two_ref.at[way, :, cols], two_send.at[layer, k, way], two_recv.at[layer, k, way], way)

    def near(k, way):
        cols = cols_of(k)
        return remote(term_ref.at[rows_of(me), cols], all_hbm.at[rows_of(me), cols], near_send.at[k, way], near_recv.at[k, way], way)

    def far(k, way):
        cols = cols_of(k)
        block = all_hbm.at[rows_of(ways[1 - way], way), cols]
        return remote(block, block, far_send.at[k, way], far_recv.at[k, way], way)

    def keep(layer, k):
        cols = cols_of(k)
        target = all_hbm.at[rows_of(me), cols] if layer else own_hbm.at[:, cols]
        return pltpu.make_async_copy(term_ref.at[rows_of(me), cols], target, keep_sem.at[layer, k])

    def start_one(layer, k):
        for way in range(2):
            one(layer, k, way).start()

    def start_two(layer, k):
        cols = cols_of(k)
        for way in range(2):
            one(layer, k, way).wait()
            rows = rows_of(ways[way], way)
            term_ref[rows, cols] = (term_ref[rows, cols].astype(F32) + one_ref[way, :, cols].astype(F32)).astype(BF16)
        for way in range(2):
            two(layer, k, way).start()

    def finish(layer, k):
        cols = cols_of(k)
        rows = rows_of(me)
        for way in range(2):
            two(layer, k, way).wait()
        term_ref[rows, cols] = (term_ref[rows, cols].astype(F32) + two_ref[0, :, cols].astype(F32) + two_ref[1, :, cols].astype(F32)).astype(BF16)
        if layer:
            for way in range(2):
                near(k, way).start()
        keep(layer, k).start()

    def start_far(k):
        for way in range(2):
            near(k, way).wait()
        keep(1, k).wait()
        for way in range(2):
            far(k, way).start()

    def when(condition, action, *args):
        if isinstance(condition, bool):
            if condition:
                action(*args)
        else:
            pl.when(condition)(lambda: action(*args))

    def meanwhile(layer, k):
        when(k >= 2, finish, layer, k - 2)
        when(k >= 1, start_two, layer, k - 1)
        if not layer:
            start_far(k)

    def weight_copies(layer):
        copies = []
        for k, width in enumerate(widths):
            for source, offset in ((wg_hbm, 0), (wu_hbm, width)):
                copies.append((source.at[layer, :, pl.ds(k * WIDE, width)], wgu_ref.at[layer, :, pl.ds(2 * k * WIDE + offset, width)]))
        copies.append((wd_hbm.at[layer], wd_ref.at[layer]))
        return [pltpu.make_async_copy(source, target, w_sem.at[layer, i]) for i, (source, target) in enumerate(copies)]

    def x_copy(t, target):
        return pltpu.make_async_copy(x_hbm.at[0, at(t, ROWS)], target.at[at(t, ROWS)], x_sem.at[t])

    dy_copy = pltpu.make_async_copy(dy_hbm.at[0], g_ref, dy_sem)
    steps = tokens // ROWS
    for copy in weight_copies(0):
        copy.start()
    for t in range(steps):
        x_copy(t, h_ref).start()
    dy_copy.start()
    for layer in range(1, layers):
        for copy in weight_copies(layer):
            copy.start()
    for copy in weight_copies(0):
        copy.wait()

    def forward(t, carry):
        rows = at(t, ROWS)
        x_copy(t, h_ref).wait()
        x = h_ref[rows, :]
        a = normed(x)
        for k, width in enumerate(widths):
            gu = dot(a, wgu_ref[0, :, pl.ds(2 * k * WIDE, 2 * width)])
            gate, up = gu[:, :width], gu[:, width:]
            mid_ref[:, pl.ds(k * WIDE, width)] = (gate * jax.nn.sigmoid(gate) * up).astype(BF16)
        h = (x.astype(F32) + dot(mid_ref[...], wd_ref[0]).astype(BF16).astype(F32)).astype(BF16)
        h_ref[rows, :] = h
        a = normed(h)
        a_ref[rows, :] = a
        at_ref[:, rows] = a.T
        return carry

    lax.fori_loop(0, steps, forward, 0)
    dy_copy.wait()

    def turn(t, carry):
        rows = at(t, ROWS)
        gt_ref[:, rows] = g_ref[rows, :].T
        return carry

    lax.fori_loop(0, steps, turn, 0)
    for layer in range(1, layers):
        for copy in weight_copies(layer):
            copy.wait()

    def chunk(layer, k, width, first, last):
        gu_cols = pl.ds(pl.multiple_of(k * 2 * WIDE, 2 * WIDE), 2 * width)
        down_rows = pl.ds(pl.multiple_of(k * WIDE, WIDE), width)

        def hidden(t, carry):
            rows = at(t, TILE)
            gu = dot(a_ref[rows, :], wgu_ref[layer, :, gu_cols])
            dh = dot_t(g_ref[rows, :], wd_ref[layer, down_rows, :]).astype(BF16).astype(F32)
            gate, up = gu[:, :width], gu[:, width:]
            s = jax.nn.sigmoid(gate)
            silu = gate * s
            hid_ref[rows, pl.ds(0, width)] = (silu * up).astype(BF16)
            dgu_ref[rows, pl.ds(width, width)] = (dh * silu).astype(BF16)
            dgu_ref[rows, pl.ds(0, width)] = (dh * up * (s + silu * (1.0 - s))).astype(BF16)
            return carry

        lax.fori_loop(0, tokens // TILE, hidden, 0)
        meanwhile(layer, k)
        dgu = dot(at_ref[...], dgu_ref[:, pl.ds(0, 2 * width)]).astype(BF16)
        down = dot(gt_ref[...], hid_ref[:, pl.ds(0, width)]).astype(BF16)
        for j in range(width // LANES):
            for i, piece in enumerate((dgu[:, j * LANES : (j + 1) * LANES], dgu[:, width + j * LANES : width + (j + 1) * LANES], down[:, j * LANES : (j + 1) * LANES])):
                term_ref[:, pl.ds(pl.multiple_of(k * 3 * WIDE, 3 * WIDE) + (3 * j + i) * LANES, LANES)] = piece
        start_one(layer, k)
        if layer:

            def by_a(t, carry):
                rows = at(t, TILE)
                part = dot_t(dgu_ref[rows, pl.ds(0, 2 * width)], wgu_ref[layer, :, gu_cols])
                if first is True:
                    da_ref[rows, :] = part
                else:
                    da_ref[rows, :] += part
                return carry

            lax.fori_loop(0, tokens // TILE, by_a, 0)

    def backward(layer):
        if layer:
            chunk(layer, 0, WIDE, True, False)

            def body(k, carry):
                chunk(layer, k, WIDE, False, False)
                return carry

            lax.fori_loop(1, full, body, 0)
        else:

            def body(k, carry):
                chunk(layer, k, WIDE, False, False)
                return carry

            lax.fori_loop(0, full, body, 0)
        for k in range(full, len(widths)):
            chunk(layer, k, widths[k], False, True)

    last = len(widths) - 1
    pl.semaphore_wait(barrier, 2)
    backward(1)
    finish(1, last - 1)
    start_two(1, last)

    for t in range(steps):
        x_copy(t, a_ref).start()

    def between(t, carry):
        rows = at(t, ROWS)
        x_copy(t, a_ref).wait()
        da = da_ref[rows, :].astype(BF16).astype(F32)
        h = h_ref[rows, :].astype(F32)
        r = scale_of(h)
        inner = jnp.mean(da * h, -1, keepdims=True)
        dh = (r * (da - h * (r * r * inner))).astype(BF16).astype(F32)
        g = (g_ref[rows, :].astype(F32) + dh).astype(BF16)
        g_ref[rows, :] = g
        gt_ref[:, rows] = g.T
        a = normed(a_ref[rows, :])
        a_ref[rows, :] = a
        at_ref[:, rows] = a.T
        return carry

    lax.fori_loop(0, steps, between, 0)
    finish(1, last)
    backward(0)
    finish(0, last - 1)
    start_two(0, last)
    finish(0, last)
    for k in range(len(widths)):
        keep(0, k).wait()
        for way in range(2):
            far(k, way).wait()


def main_call(n, x, dy, wg, wu, wd):
    layers, d, ff = wg.shape
    tokens = x.shape[1]
    if layers != 2 or n != 4:
        raise ValueError("unsupported sizes")
    chunks = -(-ff // WIDE)
    any_ = pl.BlockSpec(memory_space=pl.ANY)
    share = d // n
    sems = pltpu.SemaphoreType.DMA
    return pl.pallas_call(
        functools.partial(main_kernel, n),
        out_shape=[jax.ShapeDtypeStruct((d, 3 * ff), BF16), jax.ShapeDtypeStruct((share, 3 * ff), BF16)],
        in_specs=[any_] * 5,
        out_specs=[any_] * 2,
        scratch_shapes=[
            pltpu.VMEM((tokens, d), BF16),
            pltpu.VMEM((tokens, d), BF16),
            pltpu.VMEM((d, tokens), BF16),
            pltpu.VMEM((tokens, d), BF16),
            pltpu.VMEM((d, tokens), BF16),
            pltpu.VMEM((tokens, d), F32),
            pltpu.VMEM((layers, d, 2 * ff), BF16),
            pltpu.VMEM((layers, ff, d), BF16),
            pltpu.VMEM((ROWS, ff), BF16),
            pltpu.VMEM((tokens, WIDE), BF16),
            pltpu.VMEM((tokens, 2 * WIDE), BF16),
            pltpu.VMEM((d, 3 * ff), BF16),
            pltpu.VMEM((2, share // 2, 3 * ff), BF16),
            pltpu.VMEM((2, share, 3 * ff), BF16),
            sems((layers, 2 * chunks + 1)),
            sems((tokens // ROWS,)),
            sems,
            *[sems((layers, chunks, 2))] * 4,
            *[sems((chunks, 2))] * 4,
            sems((layers, chunks)),
        ],
        compiler_params=pltpu.CompilerParams(vmem_limit_bytes=67_000_000, collective_id=0, has_side_effects=True),
        name="main",
    )(x, dy, wg, wu, wd)


def adamw(w, m, v, g):
    m = 0.9 * m + 0.1 * g
    v = 0.95 * v + 0.05 * g * g
    step = m * lax.rsqrt(v + 1e-8) + 0.1 * w
    return (w - 0.02 * step).astype(BF16), m, v


def adam_kernel(sources, where, *refs):
    count = sum(parts for _, parts in sources)
    ins, outs = refs[count : count + 9], refs[-9:]
    ff = ins[0].shape[-1]
    start = 0
    for steps, parts in sources:
        mine, refs = refs[:parts], refs[parts:]

        @pl.when((pl.program_id(0) >= start) & (pl.program_id(0) < start + steps))
        def _(mine=mine):
            for j in range(ff // LANES):
                cols = pl.ds(j * LANES, LANES)
                for i in range(3):
                    g = [ref[:, pl.ds((3 * j + i) * LANES, LANES)].astype(F32) for ref in mine]
                    g = jnp.concatenate(g, 0) if len(g) > 1 else g[0]
                    index = (0, slice(None), cols)
                    if i == 2:
                        g, index = g.T, (0, cols, slice(None))
                    w, m, v = adamw(ins[i][index].astype(F32), ins[3 + i][index], ins[6 + i][index], g)
                    outs[i][index], outs[3 + i][index], outs[6 + i][index] = w, m, v

        start += steps


def adam_call(sources, where, arrays, so_far=()):
    layers, d, ff = arrays[0].shape
    sources = [source if isinstance(source, tuple) else (source,) for source in sources]
    row = pl.BlockSpec((1, LANES, ff), lambda s, where: (where[s, 0], where[s, 1], 0))
    column = pl.BlockSpec((1, ff, LANES), lambda s, where: (where[s, 0], 0, where[s, 1]))
    specs = [row, row, column] * 3
    flat, g_specs, steps, start = [], [], [], 0
    for source in sources:
        size = LANES // len(source)
        blocks = source[0].shape[0] // size
        for array in source:
            flat.append(array)
            g_specs.append(pl.BlockSpec((size, 3 * ff), lambda s, where, start=start, blocks=blocks: (jnp.clip(s - start, 0, blocks - 1), 0)))
        steps.append((blocks, len(source)))
        start += blocks
    elements = start * 3 * LANES * ff
    return pl.pallas_call(
        functools.partial(adam_kernel, steps),
        grid_spec=pltpu.PrefetchScalarGridSpec(
            num_scalar_prefetch=1,
            grid=(start,),
            in_specs=g_specs + specs + [pl.BlockSpec(memory_space=pl.ANY)] * len(so_far),
            out_specs=specs,
        ),
        out_shape=[jax.ShapeDtypeStruct(a.shape, a.dtype) for a in arrays],
        input_output_aliases={1 + len(flat) + 9 + i: i for i in range(len(so_far))},
        compiler_params=pltpu.CompilerParams(vmem_limit_bytes=60_000_000),
        cost_estimate=pl.CostEstimate(flops=600 * elements, bytes_accessed=22 * elements, transcendentals=elements),
        name="adam",
    )(where, *flat, *arrays, *so_far)


def solution(mesh):
    n = mesh.shape["dp"]
    ahead = [(i, (i + 1) % n) for i in range(n)]
    back = [(i, (i - 1) % n) for i in range(n)]

    def step(x, dy, *arrays):
        me = lax.axis_index("dp")

        def where(layer, *owners):
            return jnp.stack([jnp.stack([jnp.int32(layer), lax.rem(me + i, n).astype(jnp.int32)]) for i in owners])

        summed, own = main_call(n, x, dy, *arrays[:3])
        half = own.shape[0] // 2
        from_left, from_right = lax.ppermute(own, "dp", ahead), lax.ppermute(own, "dp", back)
        everyone = jnp.concatenate([jnp.array([[1, i] for i in range(n)], jnp.int32), where(0, 0)])
        new = adam_call([summed, own], everyone, arrays)
        from_left, from_right, *new = lax.optimization_barrier((from_left, from_right, *new))
        top, bottom = lax.ppermute(from_left[:half], "dp", ahead), lax.ppermute(from_right[half:], "dp", back)
        new = adam_call([from_left, from_right], where(0, n - 1, 1), arrays, new)
        return tuple(adam_call([(top, bottom)], where(0, 2), arrays, new))

    return jax.shard_map(
        step,
        mesh=mesh,
        in_specs=(P(("rep", "dp"), None, None),) * 2 + (P(None, None, None),) * 9,
        out_specs=(P("rep", None, None),) * 9,
        check_vma=False,
    )
```

```python
import functools

import jax
import jax.numpy as jnp
from jax import lax
from jax.experimental import pallas as pl
from jax.experimental.pallas import tpu as pltpu
from jax.sharding import PartitionSpec as P

BF16, F32 = jnp.bfloat16, jnp.float32
WIDE = 256
LANES = 128
TILE = 1024
FORWARD = 1024
ROWS = 512


def at(index, size):
    if isinstance(index, int):
        return pl.ds(index * size, size)
    return pl.ds(pl.multiple_of(index * size, size), size)


def dot(a, b):
    return jnp.dot(a, b, preferred_element_type=F32)


def dot_t(a, b):
    return lax.dot_general(a, b, (((1,), (1,)), ((), ())), preferred_element_type=F32)


def scale_of(wide):
    return lax.rsqrt(jnp.mean(wide * wide, -1, keepdims=True) + 1e-6)


def normed(h):
    wide = h.astype(F32)
    return (wide * scale_of(wide)).astype(BF16)


def main_kernel(
    n, x_hbm, dy_hbm, wg_hbm, wu_hbm, wd_hbm,
    all_hbm, own_hbm,
    h_ref, a_ref, at_ref, g_ref, gt_ref, da_ref, wgu_ref, wd_ref, mid_ref, hid_ref, dgu_ref, term_ref, one_ref, two_ref,
    w_sem, x_sem, dy_sem, one_send, one_recv, two_send, two_recv, near_send, near_recv, far_send, far_recv, keep_sem,
):
    tokens, d = h_ref.shape
    layers, ff, _ = wd_ref.shape
    full = ff // WIDE
    widths = [WIDE] * full + ([ff % WIDE] if ff % WIDE else [])
    share = d // n
    half = share // 2
    me = lax.axis_index("dp")
    right, left, across = (lax.rem(me + i, n) for i in (1, n - 1, 2))
    ways = (right, left)

    barrier = pltpu.get_barrier_semaphore()
    for way in ways:
        pl.semaphore_signal(barrier, inc=1, device_id={"dp": way}, device_id_type=pl.DeviceIdType.MESH)

    def cols_of(k):
        return pl.ds(pl.multiple_of(k * 3 * WIDE, 3 * WIDE), 3 * widths[k] if isinstance(k, int) else 3 * WIDE)

    def rows_of(owner, part=None):
        if part is None:
            return pl.ds(pl.multiple_of(owner * share, share), share)
        return pl.ds(pl.multiple_of(owner * share + part * half, half), half)

    def remote(source, target, send, recv, way):
        return pltpu.make_async_remote_copy(
            src_ref=source, dst_ref=target, send_sem=send, recv_sem=recv, device_id={"dp": ways[way]}, device_id_type=pl.DeviceIdType.MESH
        )

    def one(layer, k, way):
        cols = cols_of(k)
        return remote(term_ref.at[rows_of(across, way), cols], one_ref.at[way, :, cols], one_send.at[layer, k, way], one_recv.at[layer, k, way], way)

    def two(layer, k, way):
        cols = cols_of(k)
        return remote(term_ref.at[rows_of(ways[way]), cols], two_ref.at[way, :, cols], two_send.at[layer, k, way], two_recv.at[layer, k, way], way)

    def near(k, way):
        cols = cols_of(k)
        return remote(term_ref.at[rows_of(me), cols], all_hbm.at[rows_of(me), cols], near_send.at[k, way], near_recv.at[k, way], way)

    def far(k, way):
        cols = cols_of(k)
        block = all_hbm.at[rows_of(ways[1 - way], way), cols]
        return remote(block, block, far_send.at[k, way], far_recv.at[k, way], way)

    def keep(layer, k):
        cols = cols_of(k)
        target = all_hbm.at[rows_of(me), cols] if layer else own_hbm.at[:, cols]
        return pltpu.make_async_copy(term_ref.at[rows_of(me), cols], target, keep_sem.at[layer, k])

    def start_one(layer, k):
        for way in range(2):
            one(layer, k, way).start()

    def start_two(layer, k):
        cols = cols_of(k)
        for way in range(2):
            one(layer, k, way).wait()
            rows = rows_of(ways[way], way)
            term_ref[rows, cols] = (term_ref[rows, cols].astype(F32) + one_ref[way, :, cols].astype(F32)).astype(BF16)
        for way in range(2):
            two(layer, k, way).start()

    def finish(layer, k):
        cols = cols_of(k)
        rows = rows_of(me)
        for way in range(2):
            two(layer, k, way).wait()
        term_ref[rows, cols] = (term_ref[rows, cols].astype(F32) + two_ref[0, :, cols].astype(F32) + two_ref[1, :, cols].astype(F32)).astype(BF16)
        if layer:
            for way in range(2):
                near(k, way).start()
        keep(layer, k).start()

    def start_far(k):
        for way in range(2):
            near(k, way).wait()
        keep(1, k).wait()
        for way in range(2):
            far(k, way).start()

    def when(condition, action, *args):
        if isinstance(condition, bool):
            if condition:
                action(*args)
        else:
            pl.when(condition)(lambda: action(*args))

    def weight_copies(layer):
        copies = []
        for k, width in enumerate(widths):
            for source, offset in ((wg_hbm, 0), (wu_hbm, width)):
                copies.append((source.at[layer, :, pl.ds(k * WIDE, width)], wgu_ref.at[layer, :, pl.ds(2 * k * WIDE + offset, width)]))
        copies.append((wd_hbm.at[layer], wd_ref.at[layer]))
        return [pltpu.make_async_copy(source, target, w_sem.at[layer, i]) for i, (source, target) in enumerate(copies)]

    def x_copy(t, target):
        return pltpu.make_async_copy(x_hbm.at[0, at(t, ROWS)], target.at[at(t, ROWS)], x_sem.at[t])

    dy_copy = pltpu.make_async_copy(dy_hbm.at[0], g_ref, dy_sem)
    steps = tokens // ROWS
    for copy in weight_copies(0):
        copy.start()
    for t in range(steps):
        x_copy(t, h_ref).start()
    dy_copy.start()
    for layer in range(1, layers):
        for copy in weight_copies(layer):
            copy.start()
    for copy in weight_copies(0):
        copy.wait()

    def forward(t, carry):
        rows = at(t, FORWARD)
        for i in range(FORWARD // ROWS):
            x_copy(t * (FORWARD // ROWS) + i, h_ref).wait()
        x = h_ref[rows, :]
        a = normed(x)
        for k, width in enumerate(widths):
            gu = dot(a, wgu_ref[0, :, pl.ds(2 * k * WIDE, 2 * width)])
            gate, up = gu[:, :width], gu[:, width:]
            mid_ref[:, pl.ds(k * WIDE, width)] = (gate * jax.nn.sigmoid(gate) * up).astype(BF16)
        h = (x.astype(F32) + dot(mid_ref[...], wd_ref[0]).astype(BF16).astype(F32)).astype(BF16)
        h_ref[rows, :] = h
        a = normed(h)
        a_ref[rows, :] = a
        at_ref[:, rows] = a.T
        return carry

    lax.fori_loop(0, tokens // FORWARD, forward, 0)
    dy_copy.wait()

    def turn(t, carry):
        rows = at(t, ROWS)
        gt_ref[:, rows] = g_ref[rows, :].T
        return carry

    lax.fori_loop(0, steps, turn, 0)
    for layer in range(1, layers):
        for copy in weight_copies(layer):
            copy.wait()

    def chunk(layer, k, width, first):
        gu_cols = pl.ds(pl.multiple_of(k * 2 * WIDE, 2 * WIDE), 2 * width)
        down_rows = pl.ds(pl.multiple_of(k * WIDE, WIDE), width)

        def hidden(t, carry):
            rows = at(t, TILE)
            gu = dot(a_ref[rows, :], wgu_ref[layer, :, gu_cols])
            dh = dot_t(g_ref[rows, :], wd_ref[layer, down_rows, :]).astype(BF16).astype(F32)
            gate, up = gu[:, :width], gu[:, width:]
            s = jax.nn.sigmoid(gate)
            silu = gate * s
            hid_ref[rows, pl.ds(0, width)] = (silu * up).astype(BF16)
            dgu_ref[rows, pl.ds(width, width)] = (dh * silu).astype(BF16)
            dgu_ref[rows, pl.ds(0, width)] = (dh * up * (s + silu * (1.0 - s))).astype(BF16)
            return carry

        lax.fori_loop(0, tokens // TILE, hidden, 0)
        if layer:

            @pl.when(k == full - 1)
            def _():
                for t in range(steps):
                    x_copy(t, a_ref).start()

        else:
            when(k >= 3, finish, layer, k - 3)
            when(k + 3 < full, start_far, k + 3)
        dgu = dot(at_ref[...], dgu_ref[:, pl.ds(0, 2 * width)]).astype(BF16)
        down = dot(gt_ref[...], hid_ref[:, pl.ds(0, width)]).astype(BF16)
        for j in range(width // LANES):
            for i, piece in enumerate((dgu[:, j * LANES : (j + 1) * LANES], dgu[:, width + j * LANES : width + (j + 1) * LANES], down[:, j * LANES : (j + 1) * LANES])):
                term_ref[:, pl.ds(pl.multiple_of(k * 3 * WIDE, 3 * WIDE) + (3 * j + i) * LANES, LANES)] = piece
        start_one(layer, k)
        if layer:
            when(k == 0, start_two, layer, last)
            when((k >= 1) & (k < full), start_two, layer, k - 1)
        else:
            when(k >= 1, start_two, layer, k - 1)
        if layer:

            def by_a(t, carry):
                rows = at(t, TILE)
                part = dot_t(dgu_ref[rows, pl.ds(0, 2 * width)], wgu_ref[layer, :, gu_cols])
                if first:
                    da_ref[rows, :] = part
                else:
                    da_ref[rows, :] += part
                return carry

            lax.fori_loop(0, tokens // TILE, by_a, 0)
            when(k == 1, finish, layer, last)
            when((k >= 2) & (k < full), finish, layer, k - 2)

    last = len(widths) - 1
    pl.semaphore_wait(barrier, 2)
    chunk(1, last, widths[last], True)
    lax.fori_loop(0, full, lambda k, carry: (chunk(1, k, WIDE, False), carry)[1], 0)


    def between(t, carry):
        rows = at(t, ROWS)
        x_copy(t, a_ref).wait()
        da = da_ref[rows, :].astype(BF16).astype(F32)
        h = h_ref[rows, :].astype(F32)
        r = scale_of(h)
        inner = jnp.mean(da * h, -1, keepdims=True)
        dh = (r * (da - h * (r * r * inner))).astype(BF16).astype(F32)
        g = (g_ref[rows, :].astype(F32) + dh).astype(BF16)
        g_ref[rows, :] = g
        gt_ref[:, rows] = g.T
        a = normed(a_ref[rows, :])
        a_ref[rows, :] = a
        at_ref[:, rows] = a.T
        return carry

    lax.fori_loop(0, steps // 2, between, 0)
    start_two(1, full - 1)
    finish(1, full - 2)
    start_far(last)
    start_far(0)
    lax.fori_loop(steps // 2, steps, between, 0)
    finish(1, full - 1)
    start_far(1)
    start_far(2)
    lax.fori_loop(0, full, lambda k, carry: (chunk(0, k, WIDE, False), carry)[1], 0)
    chunk(0, last, widths[last], False)
    finish(0, last - 2)
    start_two(0, last)
    finish(0, last - 1)
    finish(0, last)
    for k in range(len(widths)):
        keep(0, k).wait()
        for way in range(2):
            far(k, way).wait()


def main_call(n, x, dy, wg, wu, wd):
    layers, d, ff = wg.shape
    tokens = x.shape[1]
    if layers != 2 or n != 4:
        raise ValueError("unsupported sizes")
    chunks = -(-ff // WIDE)
    any_ = pl.BlockSpec(memory_space=pl.ANY)
    share = d // n
    sems = pltpu.SemaphoreType.DMA
    return pl.pallas_call(
        functools.partial(main_kernel, n),
        out_shape=[jax.ShapeDtypeStruct((d, 3 * ff), BF16), jax.ShapeDtypeStruct((share, 3 * ff), BF16)],
        in_specs=[any_] * 5,
        out_specs=[any_] * 2,
        scratch_shapes=[
            pltpu.VMEM((tokens, d), BF16),
            pltpu.VMEM((tokens, d), BF16),
            pltpu.VMEM((d, tokens), BF16),
            pltpu.VMEM((tokens, d), BF16),
            pltpu.VMEM((d, tokens), BF16),
            pltpu.VMEM((tokens, d), F32),
            pltpu.VMEM((layers, d, 2 * ff), BF16),
            pltpu.VMEM((layers, ff, d), BF16),
            pltpu.VMEM((FORWARD, ff), BF16),
            pltpu.VMEM((tokens, WIDE), BF16),
            pltpu.VMEM((tokens, 2 * WIDE), BF16),
            pltpu.VMEM((d, 3 * ff), BF16),
            pltpu.VMEM((2, share // 2, 3 * ff), BF16),
            pltpu.VMEM((2, share, 3 * ff), BF16),
            sems((layers, 2 * chunks + 1)),
            sems((tokens // ROWS,)),
            sems,
            *[sems((layers, chunks, 2))] * 4,
            *[sems((chunks, 2))] * 4,
            sems((layers, chunks)),
        ],
        compiler_params=pltpu.CompilerParams(vmem_limit_bytes=67_000_000, collective_id=0, has_side_effects=True),
        name="main",
    )(x, dy, wg, wu, wd)


def adamw(w, m, v, g):
    m = 0.9 * m + 0.1 * g
    v = 0.95 * v + 0.05 * g * g
    step = m * lax.rsqrt(v + 1e-8) + 0.1 * w
    return (w - 0.02 * step).astype(BF16), m, v


def adam_kernel(sources, me, *refs):
    count = sum(parts for _, parts in sources)
    ins, outs = refs[count : count + 9], refs[-9:]
    units = ins[0].shape[-1]
    start = 0
    for steps, parts in sources:
        mine, refs = refs[:parts], refs[parts:]

        @pl.when((pl.program_id(0) >= start) & (pl.program_id(0) < start + steps))
        def _(mine=mine):
            for j in range(units // LANES):
                cols = pl.ds(j * LANES, LANES)
                for i in range(3):
                    g = [ref[:, pl.ds((3 * j + i) * LANES, LANES)].astype(F32) for ref in mine]
                    g = jnp.concatenate(g, 0) if len(g) > 1 else g[0]
                    index = (0, slice(None), cols)
                    if i == 2:
                        g, index = g.T, (0, cols, slice(None))
                    w, m, v = adamw(ins[i][index].astype(F32), ins[3 + i][index], ins[6 + i][index], g)
                    outs[i][index], outs[3 + i][index], outs[6 + i][index] = w, m, v

        start += steps


def adam_call(me, places, sources, arrays, so_far=()):
    layers, d, ff = arrays[0].shape
    sources = [source if isinstance(source, tuple) else (source,) for source in sources]

    def at_row(s, me):
        layer, place = places(s, me[0])
        return layer, place, 0

    def at_column(s, me):
        layer, place = places(s, me[0])
        return layer, 0, place

    row, column = pl.BlockSpec((1, LANES, ff), at_row), pl.BlockSpec((1, ff, LANES), at_column)
    specs = [row, row, column] * 3
    flat, g_specs, steps, start = [], [], [], 0
    for source in sources:
        size = LANES // len(source)
        blocks = source[0].shape[0] // size
        for array in source:
            flat.append(array)
            g_specs.append(pl.BlockSpec((size, 3 * ff), lambda s, me, start=start, blocks=blocks: (jnp.clip(s - start, 0, blocks - 1), 0)))
        steps.append((blocks, len(source)))
        start += blocks
    elements = start * 3 * LANES * ff
    return pl.pallas_call(
        functools.partial(adam_kernel, steps),
        grid_spec=pltpu.PrefetchScalarGridSpec(
            num_scalar_prefetch=1,
            grid=(start,),
            in_specs=g_specs + specs + [pl.BlockSpec(memory_space=pl.ANY)] * len(so_far),
            out_specs=specs,
        ),
        out_shape=[jax.ShapeDtypeStruct(a.shape, a.dtype) for a in arrays],
        input_output_aliases={1 + len(flat) + 9 + i: i for i in range(len(so_far))},
        compiler_params=pltpu.CompilerParams(vmem_limit_bytes=60_000_000),
        cost_estimate=pl.CostEstimate(flops=600 * elements, bytes_accessed=22 * elements, transcendentals=elements),
        name="adam",
    )(me, *flat, *arrays, *so_far)


def solution(mesh):
    n = mesh.shape["dp"]
    ahead = [(i, (i + 1) % n) for i in range(n)]
    back = [(i, (i - 1) % n) for i in range(n)]

    def step(x, dy, *arrays):
        me = lax.axis_index("dp").astype(jnp.int32)[None]

        def place(*steps):
            return lambda s, me: (0, lax.rem(me + steps[0] + s * (steps[-1] - steps[0]), n))

        def everyone(s, me):
            return jnp.where(s < n, 1, 0), jnp.where(s < n, s, me)

        x, me = lax.optimization_barrier((x, me))
        summed, own = main_call(n, x, dy, *arrays[:3])
        half = own.shape[0] // 2
        from_left, from_right = lax.ppermute(own, "dp", ahead), lax.ppermute(own, "dp", back)
        new = adam_call(me, everyone, [summed, own], arrays)
        from_left, from_right, *new = lax.optimization_barrier((from_left, from_right, *new))
        top, bottom = lax.ppermute(from_left[:half], "dp", ahead), lax.ppermute(from_right[half:], "dp", back)
        new = adam_call(me, place(n - 1, n + 1), [from_left, from_right], arrays, new)
        return tuple(adam_call(me, place(2), [(top, bottom)], arrays, new))

    return jax.shard_map(
        step,
        mesh=mesh,
        in_specs=(P(("rep", "dp"), None, None),) * 2 + (P(None, None, None),) * 9,
        out_specs=(P("rep", None, None),) * 9,
        check_vma=False,
    )
```

```python
import functools

import jax
import jax.numpy as jnp
from jax import lax
from jax.experimental import pallas as pl
from jax.experimental.pallas import tpu as pltpu
from jax.sharding import PartitionSpec as P

BF16, F32 = jnp.bfloat16, jnp.float32
WIDE = 256
LANES = 128
TILE = 1024
FORWARD = 1024
ROWS = 512


def at(index, size):
    if isinstance(index, int):
        return pl.ds(index * size, size)
    return pl.ds(pl.multiple_of(index * size, size), size)


def dot(a, b):
    return jnp.dot(a, b, preferred_element_type=F32)


def dot_t(a, b):
    return lax.dot_general(a, b, (((1,), (1,)), ((), ())), preferred_element_type=F32)


def scale_of(wide):
    return lax.rsqrt(jnp.mean(wide * wide, -1, keepdims=True) + 1e-6)


def normed(h):
    wide = h.astype(F32)
    return (wide * scale_of(wide)).astype(BF16)


def main_kernel(
    n, x_hbm, dy_hbm, wg_hbm, wu_hbm, wd_hbm,
    all_hbm, own_hbm,
    h_ref, a_ref, at_ref, g_ref, gt_ref, da_ref, wgu_ref, wd_ref, hid_ref, dgu_ref, term_ref, one_ref, two_ref,
    w_sem, x_sem, dy_sem, one_send, one_recv, two_send, two_recv, near_send, near_recv, far_send, far_recv, keep_sem,
):
    tokens, d = h_ref.shape
    layers, ff, _ = wd_ref.shape
    full = ff // WIDE
    widths = [WIDE] * full + ([ff % WIDE] if ff % WIDE else [])
    share = d // n
    half = share // 2
    me = lax.axis_index("dp")
    right, left, across = (lax.rem(me + i, n) for i in (1, n - 1, 2))
    ways = (right, left)

    barrier = pltpu.get_barrier_semaphore()
    for way in ways:
        pl.semaphore_signal(barrier, inc=1, device_id={"dp": way}, device_id_type=pl.DeviceIdType.MESH)

    def cols_of(k):
        return pl.ds(pl.multiple_of(k * 3 * WIDE, 3 * WIDE), 3 * widths[k] if isinstance(k, int) else 3 * WIDE)

    def rows_of(owner, part=None):
        if part is None:
            return pl.ds(pl.multiple_of(owner * share, share), share)
        return pl.ds(pl.multiple_of(owner * share + part * half, half), half)

    def remote(source, target, send, recv, way):
        return pltpu.make_async_remote_copy(
            src_ref=source, dst_ref=target, send_sem=send, recv_sem=recv, device_id={"dp": ways[way]}, device_id_type=pl.DeviceIdType.MESH
        )

    def one(layer, k, way):
        cols = cols_of(k)
        return remote(term_ref.at[rows_of(across, way), cols], one_ref.at[way, :, cols], one_send.at[layer, k, way], one_recv.at[layer, k, way], way)

    def two(layer, k, way):
        cols = cols_of(k)
        return remote(term_ref.at[rows_of(ways[way]), cols], two_ref.at[way, :, cols], two_send.at[layer, k, way], two_recv.at[layer, k, way], way)

    def near(k, way):
        cols = cols_of(k)
        return remote(term_ref.at[rows_of(me), cols], all_hbm.at[rows_of(me), cols], near_send.at[k, way], near_recv.at[k, way], way)

    def far(k, way):
        cols = cols_of(k)
        block = all_hbm.at[rows_of(ways[1 - way], way), cols]
        return remote(block, block, far_send.at[k, way], far_recv.at[k, way], way)

    def keep(layer, k):
        cols = cols_of(k)
        target = all_hbm.at[rows_of(me), cols] if layer else own_hbm.at[:, cols]
        return pltpu.make_async_copy(term_ref.at[rows_of(me), cols], target, keep_sem.at[layer, k])

    def start_one(layer, k):
        for way in range(2):
            one(layer, k, way).start()

    def start_two(layer, k):
        cols = cols_of(k)
        for way in range(2):
            one(layer, k, way).wait()
            rows = rows_of(ways[way], way)
            term_ref[rows, cols] = (term_ref[rows, cols].astype(F32) + one_ref[way, :, cols].astype(F32)).astype(BF16)
        for way in range(2):
            two(layer, k, way).start()

    def finish(layer, k):
        cols = cols_of(k)
        rows = rows_of(me)
        for way in range(2):
            two(layer, k, way).wait()
        term_ref[rows, cols] = (term_ref[rows, cols].astype(F32) + two_ref[0, :, cols].astype(F32) + two_ref[1, :, cols].astype(F32)).astype(BF16)
        if layer:
            for way in range(2):
                near(k, way).start()
        keep(layer, k).start()

    def start_far(k):
        for way in range(2):
            near(k, way).wait()
        keep(1, k).wait()
        for way in range(2):
            far(k, way).start()

    def when(condition, action, *args):
        if isinstance(condition, bool):
            if condition:
                action(*args)
        else:
            pl.when(condition)(lambda: action(*args))

    def weight_copies(layer):
        copies = []
        for k, width in enumerate(widths):
            for source, offset in ((wg_hbm, 0), (wu_hbm, width)):
                copies.append((source.at[layer, :, pl.ds(k * WIDE, width)], wgu_ref.at[layer, :, pl.ds(2 * k * WIDE + offset, width)]))
        copies.append((wd_hbm.at[layer], wd_ref.at[layer]))
        return [pltpu.make_async_copy(source, target, w_sem.at[layer, i]) for i, (source, target) in enumerate(copies)]

    def x_copy(t, target):
        return pltpu.make_async_copy(x_hbm.at[0, at(t, ROWS)], target.at[at(t, ROWS)], x_sem.at[t])

    dy_copy = pltpu.make_async_copy(dy_hbm.at[0], g_ref, dy_sem)
    steps = tokens // ROWS
    for copy in weight_copies(0):
        copy.start()
    for t in range(steps):
        x_copy(t, h_ref).start()
    dy_copy.start()
    for layer in range(1, layers):
        for copy in weight_copies(layer):
            copy.start()
    for copy in weight_copies(0):
        copy.wait()

    def forward(t, carry):
        rows = at(t, FORWARD)
        for i in range(FORWARD // ROWS):
            x_copy(t * (FORWARD // ROWS) + i, h_ref).wait()
        x = h_ref[rows, :]
        a = normed(x)
        for k, width in enumerate(widths):
            gu = dot(a, wgu_ref[0, :, pl.ds(2 * k * WIDE, 2 * width)])
            gate, up = gu[:, :width], gu[:, width:]
            dgu_ref[pl.ds(k // 2 * FORWARD, FORWARD), pl.ds(k % 2 * WIDE, width)] = (gate * jax.nn.sigmoid(gate) * up).astype(BF16)
        down = 0.0
        for k in range(0, len(widths), 2):
            width = sum(widths[k : k + 2])
            down += dot(dgu_ref[pl.ds(k // 2 * FORWARD, FORWARD), pl.ds(0, width)], wd_ref[0, pl.ds(k * WIDE, width), :])
        h = (x.astype(F32) + down.astype(BF16).astype(F32)).astype(BF16)
        h_ref[rows, :] = h
        a = normed(h)
        a_ref[rows, :] = a
        at_ref[:, rows] = a.T
        return carry

    lax.fori_loop(0, tokens // FORWARD, forward, 0)
    dy_copy.wait()

    def turn(t, carry):
        rows = at(t, ROWS)
        gt_ref[:, rows] = g_ref[rows, :].T
        return carry

    lax.fori_loop(0, steps, turn, 0)
    for layer in range(1, layers):
        for copy in weight_copies(layer):
            copy.wait()

    def chunk(layer, k, width, first):
        gu_cols = pl.ds(pl.multiple_of(k * 2 * WIDE, 2 * WIDE), 2 * width)
        down_rows = pl.ds(pl.multiple_of(k * WIDE, WIDE), width)

        def hidden(t, carry):
            rows = at(t, 2 * TILE)
            gu = dot(a_ref[rows, :], wgu_ref[layer, :, gu_cols])
            dh = dot_t(g_ref[rows, :], wd_ref[layer, down_rows, :]).astype(BF16).astype(F32)
            gate, up = gu[:, :width], gu[:, width:]
            s = jax.nn.sigmoid(gate)
            silu = gate * s
            hid_ref[rows, pl.ds(0, width)] = (silu * up).astype(BF16)
            dgu_ref[rows, pl.ds(width, width)] = (dh * silu).astype(BF16)
            dgu_ref[rows, pl.ds(0, width)] = (dh * up * (s + silu * (1.0 - s))).astype(BF16)
            return carry

        lax.fori_loop(0, tokens // (2 * TILE), hidden, 0)
        if layer:
            when(k == 0, start_two, layer, last)
            when((k >= 1) & (k < full), start_two, layer, k - 1)

            @pl.when(k == full - 1)
            def _():
                for t in range(steps):
                    x_copy(t, a_ref).start()

        else:
            when(k >= 3, finish, layer, k - 3)
            when(k + 3 < full, start_far, k + 3)
        dgu = dot(at_ref[...], dgu_ref[:, pl.ds(0, 2 * width)]).astype(BF16)
        down = dot(gt_ref[...], hid_ref[:, pl.ds(0, width)]).astype(BF16)
        for j in range(width // LANES):
            for i, piece in enumerate((dgu[:, j * LANES : (j + 1) * LANES], dgu[:, width + j * LANES : width + (j + 1) * LANES], down[:, j * LANES : (j + 1) * LANES])):
                term_ref[:, pl.ds(pl.multiple_of(k * 3 * WIDE, 3 * WIDE) + (3 * j + i) * LANES, LANES)] = piece
        start_one(layer, k)
        if not layer:
            when(k >= 1, start_two, layer, k - 1)
        if layer:

            def by_a(t, carry):
                rows = at(t, TILE)
                part = dot_t(dgu_ref[rows, pl.ds(0, 2 * width)], wgu_ref[layer, :, gu_cols])
                if first:
                    da_ref[rows, :] = part
                else:
                    da_ref[rows, :] += part
                return carry

            lax.fori_loop(0, tokens // TILE, by_a, 0)
            when(k == 0, finish, layer, last)
            when((k >= 2) & (k < full), finish, layer, k - 2)

    last = len(widths) - 1
    pl.semaphore_wait(barrier, 2)
    chunk(1, last, widths[last], True)
    lax.fori_loop(0, full, lambda k, carry: (chunk(1, k, WIDE, False), carry)[1], 0)


    def between(t, carry):
        rows = at(t, ROWS)
        x_copy(t, a_ref).wait()
        da = da_ref[rows, :].astype(BF16).astype(F32)
        h = h_ref[rows, :].astype(F32)
        r = scale_of(h)
        inner = jnp.mean(da * h, -1, keepdims=True)
        dh = (r * (da - h * (r * r * inner))).astype(BF16).astype(F32)
        g = (g_ref[rows, :].astype(F32) + dh).astype(BF16)
        g_ref[rows, :] = g
        gt_ref[:, rows] = g.T
        a = normed(a_ref[rows, :])
        a_ref[rows, :] = a
        at_ref[:, rows] = a.T
        return carry

    lax.fori_loop(0, steps // 4, between, 0)
    start_two(1, full - 1)
    finish(1, full - 2)
    start_far(last)
    start_far(0)
    lax.fori_loop(steps // 4, steps, between, 0)
    finish(1, full - 1)
    start_far(1)
    start_far(2)
    lax.fori_loop(0, full, lambda k, carry: (chunk(0, k, WIDE, False), carry)[1], 0)
    chunk(0, last, widths[last], False)
    finish(0, last - 2)
    start_two(0, last)
    finish(0, last - 1)
    finish(0, last)
    for k in range(len(widths)):
        keep(0, k).wait()
        for way in range(2):
            far(k, way).wait()


def main_call(n, x, dy, wg, wu, wd):
    layers, d, ff = wg.shape
    tokens = x.shape[1]
    if layers != 2 or n != 4:
        raise ValueError("unsupported sizes")
    chunks = -(-ff // WIDE)
    any_ = pl.BlockSpec(memory_space=pl.ANY)
    share = d // n
    sems = pltpu.SemaphoreType.DMA
    return pl.pallas_call(
        functools.partial(main_kernel, n),
        out_shape=[jax.ShapeDtypeStruct((d, 3 * ff), BF16), jax.ShapeDtypeStruct((share, 3 * ff), BF16)],
        in_specs=[any_] * 5,
        out_specs=[any_] * 2,
        scratch_shapes=[
            pltpu.VMEM((tokens, d), BF16),
            pltpu.VMEM((tokens, d), BF16),
            pltpu.VMEM((d, tokens), BF16),
            pltpu.VMEM((tokens, d), BF16),
            pltpu.VMEM((d, tokens), BF16),
            pltpu.VMEM((tokens, d), F32),
            pltpu.VMEM((layers, d, 2 * ff), BF16),
            pltpu.VMEM((layers, ff, d), BF16),
            pltpu.VMEM((tokens, WIDE), BF16),
            pltpu.VMEM((tokens, 2 * WIDE), BF16),
            pltpu.VMEM((d, 3 * ff), BF16),
            pltpu.VMEM((2, share // 2, 3 * ff), BF16),
            pltpu.VMEM((2, share, 3 * ff), BF16),
            sems((layers, 2 * chunks + 1)),
            sems((tokens // ROWS,)),
            sems,
            *[sems((layers, chunks, 2))] * 4,
            *[sems((chunks, 2))] * 4,
            sems((layers, chunks)),
        ],
        compiler_params=pltpu.CompilerParams(vmem_limit_bytes=67_000_000, collective_id=0, has_side_effects=True),
        name="main",
    )(x, dy, wg, wu, wd)


def adamw(w, m, v, g):
    m = 0.9 * m + 0.1 * g
    v = 0.95 * v + 0.05 * g * g
    step = m * lax.rsqrt(v + 1e-8) + 0.1 * w
    return (w - 0.02 * step).astype(BF16), m, v


def adam_kernel(sources, me, *refs):
    count = sum(parts for _, parts in sources)
    ins, outs = refs[count : count + 9], refs[-9:]
    units = ins[0].shape[-1]
    start = 0
    for steps, parts in sources:
        mine, refs = refs[:parts], refs[parts:]

        @pl.when((pl.program_id(0) >= start) & (pl.program_id(0) < start + steps))
        def _(mine=mine):
            for j in range(units // LANES):
                cols = pl.ds(j * LANES, LANES)
                for i in range(3):
                    g = [ref[:, pl.ds((3 * j + i) * LANES, LANES)].astype(F32) for ref in mine]
                    g = jnp.concatenate(g, 0) if len(g) > 1 else g[0]
                    index = (0, slice(None), cols)
                    if i == 2:
                        g, index = g.T, (0, cols, slice(None))
                    w, m, v = adamw(ins[i][index].astype(F32), ins[3 + i][index], ins[6 + i][index], g)
                    outs[i][index], outs[3 + i][index], outs[6 + i][index] = w, m, v

        start += steps


def adam_call(me, places, sources, arrays, so_far=()):
    layers, d, ff = arrays[0].shape
    sources = [source if isinstance(source, tuple) else (source,) for source in sources]

    def at_row(s, me):
        layer, place = places(s, me[0])
        return layer, place, 0

    def at_column(s, me):
        layer, place = places(s, me[0])
        return layer, 0, place

    row, column = pl.BlockSpec((1, LANES, ff), at_row), pl.BlockSpec((1, ff, LANES), at_column)
    specs = [row, row, column] * 3
    flat, g_specs, steps, start = [], [], [], 0
    for source in sources:
        size = LANES // len(source)
        blocks = source[0].shape[0] // size
        for array in source:
            flat.append(array)
            g_specs.append(pl.BlockSpec((size, 3 * ff), lambda s, me, start=start, blocks=blocks: (jnp.clip(s - start, 0, blocks - 1), 0)))
        steps.append((blocks, len(source)))
        start += blocks
    elements = start * 3 * LANES * ff
    return pl.pallas_call(
        functools.partial(adam_kernel, steps),
        grid_spec=pltpu.PrefetchScalarGridSpec(
            num_scalar_prefetch=1,
            grid=(start,),
            in_specs=g_specs + specs + [pl.BlockSpec(memory_space=pl.ANY)] * len(so_far),
            out_specs=specs,
        ),
        out_shape=[jax.ShapeDtypeStruct(a.shape, a.dtype) for a in arrays],
        input_output_aliases={1 + len(flat) + 9 + i: i for i in range(len(so_far))},
        compiler_params=pltpu.CompilerParams(vmem_limit_bytes=60_000_000),
        cost_estimate=pl.CostEstimate(flops=600 * elements, bytes_accessed=22 * elements, transcendentals=elements),
        name="adam",
    )(me, *flat, *arrays, *so_far)


def solution(mesh):
    n = mesh.shape["dp"]
    ahead = [(i, (i + 1) % n) for i in range(n)]
    back = [(i, (i - 1) % n) for i in range(n)]

    def step(x, dy, *arrays):
        me = lax.axis_index("dp").astype(jnp.int32)[None]

        def place(*steps):
            return lambda s, me: (0, lax.rem(me + steps[0] + s * (steps[-1] - steps[0]), n))

        def everyone(s, me):
            return jnp.where(s < n, 1, 0), jnp.where(s < n, s, me)

        x, me = lax.optimization_barrier((x, me))
        summed, own = main_call(n, x, dy, *arrays[:3])
        half = own.shape[0] // 2
        from_left, from_right = lax.ppermute(own, "dp", ahead), lax.ppermute(own, "dp", back)
        new = adam_call(me, everyone, [summed, own], arrays)
        from_left, from_right, *new = lax.optimization_barrier((from_left, from_right, *new))
        top, bottom = lax.ppermute(from_left[:half], "dp", ahead), lax.ppermute(from_right[half:], "dp", back)
        new = adam_call(me, place(n - 1, n + 1), [from_left, from_right], arrays, new)
        return tuple(adam_call(me, place(2), [(top, bottom)], arrays, new))

    return jax.shard_map(
        step,
        mesh=mesh,
        in_specs=(P(("rep", "dp"), None, None),) * 2 + (P(None, None, None),) * 9,
        out_specs=(P("rep", None, None),) * 9,
        check_vma=False,
    )
```

```python
import functools

import jax
import jax.numpy as jnp
from jax import lax
from jax.experimental import pallas as pl
from jax.experimental.pallas import tpu as pltpu
from jax.sharding import PartitionSpec as P

BF16, F32 = jnp.bfloat16, jnp.float32
WIDE = 256
LANES = 128
TILE = 2048
FORWARD = 1024
ROWS = 512


def at(index, size):
    if isinstance(index, int):
        return pl.ds(index * size, size)
    return pl.ds(pl.multiple_of(index * size, size), size)


def dot(a, b):
    return jnp.dot(a, b, preferred_element_type=F32)


def dot_t(a, b):
    return lax.dot_general(a, b, (((1,), (1,)), ((), ())), preferred_element_type=F32)


def scale_of(wide):
    return lax.rsqrt(jnp.mean(wide * wide, -1, keepdims=True) + 1e-6)


def normed(h):
    wide = h.astype(F32)
    return (wide * scale_of(wide)).astype(BF16)


def main_kernel(
    n, x_hbm, dy_hbm, wg_hbm, wu_hbm, wd_hbm,
    all_hbm, own_hbm,
    h_ref, a_ref, at_ref, g_ref, gt_ref, da_ref, wgu_ref, wd_ref, hid_ref, dgu_ref, term_ref, one_ref, two_ref,
    w_sem, x_sem, dy_sem, one_send, one_recv, two_send, two_recv, near_send, near_recv, far_send, far_recv, keep_sem,
):
    tokens, d = h_ref.shape
    layers, ff, _ = wd_ref.shape
    full = ff // WIDE
    widths = [WIDE] * full + ([ff % WIDE] if ff % WIDE else [])
    share = d // n
    half = share // 2
    me = lax.axis_index("dp")
    right, left, across = (lax.rem(me + i, n) for i in (1, n - 1, 2))
    ways = (right, left)

    barrier = pltpu.get_barrier_semaphore()
    for way in ways:
        pl.semaphore_signal(barrier, inc=1, device_id={"dp": way}, device_id_type=pl.DeviceIdType.MESH)

    def cols_of(k):
        return pl.ds(pl.multiple_of(k * 3 * WIDE, 3 * WIDE), 3 * widths[k] if isinstance(k, int) else 3 * WIDE)

    def rows_of(owner, part=None):
        if part is None:
            return pl.ds(pl.multiple_of(owner * share, share), share)
        return pl.ds(pl.multiple_of(owner * share + part * half, half), half)

    def remote(source, target, send, recv, way):
        return pltpu.make_async_remote_copy(
            src_ref=source, dst_ref=target, send_sem=send, recv_sem=recv, device_id={"dp": ways[way]}, device_id_type=pl.DeviceIdType.MESH
        )

    def one(layer, k, way):
        cols = cols_of(k)
        return remote(term_ref.at[rows_of(across, way), cols], one_ref.at[way, :, cols], one_send.at[layer, k, way], one_recv.at[layer, k, way], way)

    def two(layer, k, way):
        cols = cols_of(k)
        return remote(term_ref.at[rows_of(ways[way]), cols], two_ref.at[way, :, cols], two_send.at[layer, k, way], two_recv.at[layer, k, way], way)

    def near(k, way):
        cols = cols_of(k)
        return remote(term_ref.at[rows_of(me), cols], all_hbm.at[rows_of(me), cols], near_send.at[k, way], near_recv.at[k, way], way)

    def far(k, way):
        cols = cols_of(k)
        block = all_hbm.at[rows_of(ways[1 - way], way), cols]
        return remote(block, block, far_send.at[k, way], far_recv.at[k, way], way)

    def keep(layer, k):
        cols = cols_of(k)
        target = all_hbm.at[rows_of(me), cols] if layer else own_hbm.at[:, cols]
        return pltpu.make_async_copy(term_ref.at[rows_of(me), cols], target, keep_sem.at[layer, k])

    def start_one(layer, k):
        for way in range(2):
            one(layer, k, way).start()

    def start_two(layer, k):
        cols = cols_of(k)
        for way in range(2):
            one(layer, k, way).wait()
            rows = rows_of(ways[way], way)
            term_ref[rows, cols] = (term_ref[rows, cols].astype(F32) + one_ref[way, :, cols].astype(F32)).astype(BF16)
        for way in range(2):
            two(layer, k, way).start()

    def finish(layer, k):
        cols = cols_of(k)
        rows = rows_of(me)
        for way in range(2):
            two(layer, k, way).wait()
        term_ref[rows, cols] = (term_ref[rows, cols].astype(F32) + two_ref[0, :, cols].astype(F32) + two_ref[1, :, cols].astype(F32)).astype(BF16)
        if layer:
            for way in range(2):
                near(k, way).start()
        keep(layer, k).start()

    def start_far(k):
        for way in range(2):
            near(k, way).wait()
        keep(1, k).wait()
        for way in range(2):
            far(k, way).start()

    def when(condition, action, *args):
        if isinstance(condition, bool):
            if condition:
                action(*args)
        else:
            pl.when(condition)(lambda: action(*args))

    def weight_copies(layer):
        copies = []
        for k, width in enumerate(widths):
            for source, offset in ((wg_hbm, 0), (wu_hbm, width)):
                copies.append((source.at[layer, :, pl.ds(k * WIDE, width)], wgu_ref.at[layer, :, pl.ds(2 * k * WIDE + offset, width)]))
        copies.append((wd_hbm.at[layer], wd_ref.at[layer]))
        return [pltpu.make_async_copy(source, target, w_sem.at[layer, i]) for i, (source, target) in enumerate(copies)]

    def x_copy(t, target):
        return pltpu.make_async_copy(x_hbm.at[0, at(t, ROWS)], target.at[at(t, ROWS)], x_sem.at[t])

    dy_copy = pltpu.make_async_copy(dy_hbm.at[0], g_ref, dy_sem)
    steps = tokens // ROWS
    for copy in weight_copies(0):
        copy.start()
    for t in range(steps):
        x_copy(t, h_ref).start()
    dy_copy.start()
    for layer in range(1, layers):
        for copy in weight_copies(layer):
            copy.start()
    for copy in weight_copies(0):
        copy.wait()

    def forward(t, carry):
        rows = at(t, FORWARD)
        for i in range(FORWARD // ROWS):
            x_copy(t * (FORWARD // ROWS) + i, h_ref).wait()
        x = h_ref[rows, :]
        a = normed(x)
        for k, width in enumerate(widths):
            gu = dot(a, wgu_ref[0, :, pl.ds(2 * k * WIDE, 2 * width)])
            gate, up = gu[:, :width], gu[:, width:]
            dgu_ref[pl.ds(k // 2 * FORWARD, FORWARD), pl.ds(k % 2 * WIDE, width)] = (gate * jax.nn.sigmoid(gate) * up).astype(BF16)
        down = 0.0
        for k in range(0, len(widths), 2):
            width = sum(widths[k : k + 2])
            down += dot(dgu_ref[pl.ds(k // 2 * FORWARD, FORWARD), pl.ds(0, width)], wd_ref[0, pl.ds(k * WIDE, width), :])
        h = (x.astype(F32) + down.astype(BF16).astype(F32)).astype(BF16)
        h_ref[rows, :] = h
        a = normed(h)
        a_ref[rows, :] = a
        at_ref[:, rows] = a.T
        return carry

    lax.fori_loop(0, tokens // FORWARD, forward, 0)
    dy_copy.wait()

    def turn(t, carry):
        rows = at(t, ROWS)
        gt_ref[:, rows] = g_ref[rows, :].T
        return carry

    lax.fori_loop(0, steps, turn, 0)
    for layer in range(1, layers):
        for copy in weight_copies(layer):
            copy.wait()

    def chunk(layer, k, width, first):
        gu_cols = pl.ds(pl.multiple_of(k * 2 * WIDE, 2 * WIDE), 2 * width)
        down_rows = pl.ds(pl.multiple_of(k * WIDE, WIDE), width)

        def hidden(t, carry):
            rows = at(t, TILE)
            gu = dot(a_ref[rows, :], wgu_ref[layer, :, gu_cols])
            dh = dot_t(g_ref[rows, :], wd_ref[layer, down_rows, :]).astype(BF16).astype(F32)
            gate, up = gu[:, :width], gu[:, width:]
            s = jax.nn.sigmoid(gate)
            silu = gate * s
            hid_ref[rows, pl.ds(0, width)] = (silu * up).astype(BF16)
            dgu_ref[rows, pl.ds(width, width)] = (dh * silu).astype(BF16)
            dgu_ref[rows, pl.ds(0, width)] = (dh * up * (s + silu * (1.0 - s))).astype(BF16)
            return carry

        lax.fori_loop(0, tokens // TILE, hidden, 0)
        if layer:
            when(k == 0, start_two, layer, last)
            when((k >= 1) & (k < full), start_two, layer, k - 1)

            @pl.when(k == full - 1)
            def _():
                for t in range(steps):
                    x_copy(t, a_ref).start()

        else:
            when(k >= 3, finish, layer, k - 3)
            when(k + 3 < full, start_far, k + 3)
        dgu = dot(at_ref[...], dgu_ref[:, pl.ds(0, 2 * width)]).astype(BF16)
        down = dot(gt_ref[...], hid_ref[:, pl.ds(0, width)]).astype(BF16)
        for j in range(width // LANES):
            for i, piece in enumerate((dgu[:, j * LANES : (j + 1) * LANES], dgu[:, width + j * LANES : width + (j + 1) * LANES], down[:, j * LANES : (j + 1) * LANES])):
                term_ref[:, pl.ds(pl.multiple_of(k * 3 * WIDE, 3 * WIDE) + (3 * j + i) * LANES, LANES)] = piece
        start_one(layer, k)
        if not layer:
            when(k >= 1, start_two, layer, k - 1)
        if layer:

            def by_a(t, carry):
                rows = at(t, TILE)
                part = dot_t(dgu_ref[rows, pl.ds(0, 2 * width)], wgu_ref[layer, :, gu_cols])
                if first:
                    da_ref[rows, :] = part
                else:
                    da_ref[rows, :] += part
                return carry

            lax.fori_loop(0, tokens // TILE, by_a, 0)
            when(k == 0, finish, layer, last)
            when((k >= 2) & (k < full), finish, layer, k - 2)

    last = len(widths) - 1
    pl.semaphore_wait(barrier, 2)
    chunk(1, last, widths[last], True)
    lax.fori_loop(0, full, lambda k, carry: (chunk(1, k, WIDE, False), carry)[1], 0)


    def between(t, carry):
        rows = at(t, ROWS)
        x_copy(t, a_ref).wait()
        da = da_ref[rows, :].astype(BF16).astype(F32)
        h = h_ref[rows, :].astype(F32)
        r = scale_of(h)
        inner = jnp.mean(da * h, -1, keepdims=True)
        dh = (r * (da - h * (r * r * inner))).astype(BF16).astype(F32)
        g = (g_ref[rows, :].astype(F32) + dh).astype(BF16)
        g_ref[rows, :] = g
        gt_ref[:, rows] = g.T
        a = normed(a_ref[rows, :])
        a_ref[rows, :] = a
        at_ref[:, rows] = a.T
        return carry

    lax.fori_loop(0, steps // 4, between, 0)
    start_two(1, full - 1)
    finish(1, full - 2)
    start_far(last)
    start_far(0)
    lax.fori_loop(steps // 4, steps, between, 0)
    finish(1, full - 1)
    start_far(1)
    start_far(2)
    lax.fori_loop(0, full, lambda k, carry: (chunk(0, k, WIDE, False), carry)[1], 0)
    chunk(0, last, widths[last], False)
    finish(0, last - 2)
    start_two(0, last)
    finish(0, last - 1)
    finish(0, last)
    for k in range(len(widths)):
        keep(0, k).wait()
        for way in range(2):
            far(k, way).wait()


def main_call(n, x, dy, wg, wu, wd):
    layers, d, ff = wg.shape
    tokens = x.shape[1]
    if layers != 2 or n != 4:
        raise ValueError("unsupported sizes")
    chunks = -(-ff // WIDE)
    any_ = pl.BlockSpec(memory_space=pl.ANY)
    share = d // n
    sems = pltpu.SemaphoreType.DMA
    return pl.pallas_call(
        functools.partial(main_kernel, n),
        out_shape=[jax.ShapeDtypeStruct((d, 3 * ff), BF16), jax.ShapeDtypeStruct((share, 3 * ff), BF16)],
        in_specs=[any_] * 5,
        out_specs=[any_] * 2,
        scratch_shapes=[
            pltpu.VMEM((tokens, d), BF16),
            pltpu.VMEM((tokens, d), BF16),
            pltpu.VMEM((d, tokens), BF16),
            pltpu.VMEM((tokens, d), BF16),
            pltpu.VMEM((d, tokens), BF16),
            pltpu.VMEM((tokens, d), F32),
            pltpu.VMEM((layers, d, 2 * ff), BF16),
            pltpu.VMEM((layers, ff, d), BF16),
            pltpu.VMEM((tokens, WIDE), BF16),
            pltpu.VMEM((tokens, 2 * WIDE), BF16),
            pltpu.VMEM((d, 3 * ff), BF16),
            pltpu.VMEM((2, share // 2, 3 * ff), BF16),
            pltpu.VMEM((2, share, 3 * ff), BF16),
            sems((layers, 2 * chunks + 1)),
            sems((tokens // ROWS,)),
            sems,
            *[sems((layers, chunks, 2))] * 4,
            *[sems((chunks, 2))] * 4,
            sems((layers, chunks)),
        ],
        compiler_params=pltpu.CompilerParams(vmem_limit_bytes=67_000_000, collective_id=0, has_side_effects=True),
        name="main",
    )(x, dy, wg, wu, wd)


def adamw(w, m, v, g):
    m = 0.9 * m + 0.1 * g
    v = 0.95 * v + 0.05 * g * g
    step = m * lax.rsqrt(v + 1e-8) + 0.1 * w
    return (w - 0.02 * step).astype(BF16), m, v


def adam_kernel(sources, me, *refs):
    count = sum(parts for _, parts in sources)
    ins, outs = refs[count : count + 9], refs[-9:]
    units = ins[0].shape[-1]
    start = 0
    for steps, parts in sources:
        mine, refs = refs[:parts], refs[parts:]

        @pl.when((pl.program_id(0) >= start) & (pl.program_id(0) < start + steps))
        def _(mine=mine):
            def unit(j, carry, mine=mine):
                cols = at(j, LANES)
                for i in range(3):
                    g = [ref[:, at(3 * j + i, LANES)].astype(F32) for ref in mine]
                    g = jnp.concatenate(g, 0) if len(g) > 1 else g[0]
                    index = (0, slice(None), cols)
                    if i == 2:
                        g, index = g.T, (0, cols, slice(None))
                    w, m, v = adamw(ins[i][index].astype(F32), ins[3 + i][index], ins[6 + i][index], g)
                    outs[i][index], outs[3 + i][index], outs[6 + i][index] = w, m, v
                return carry

            if len(sources) == 1:
                for j in range(units // LANES):
                    unit(j, 0)
            else:
                lax.fori_loop(0, units // LANES, unit, 0)

        start += steps


def adam_call(me, places, sources, arrays, so_far=()):
    layers, d, ff = arrays[0].shape
    sources = [source if isinstance(source, tuple) else (source,) for source in sources]

    def at_row(s, me):
        layer, place = places(s, me[0])
        return layer, place, 0

    def at_column(s, me):
        layer, place = places(s, me[0])
        return layer, 0, place

    row, column = pl.BlockSpec((1, LANES, ff), at_row), pl.BlockSpec((1, ff, LANES), at_column)
    specs = [row, row, column] * 3
    flat, g_specs, steps, start = [], [], [], 0
    for source in sources:
        size = LANES // len(source)
        blocks = source[0].shape[0] // size
        for array in source:
            flat.append(array)
            g_specs.append(pl.BlockSpec((size, 3 * ff), lambda s, me, start=start, blocks=blocks: (jnp.clip(s - start, 0, blocks - 1), 0)))
        steps.append((blocks, len(source)))
        start += blocks
    elements = start * 3 * LANES * ff
    return pl.pallas_call(
        functools.partial(adam_kernel, steps),
        grid_spec=pltpu.PrefetchScalarGridSpec(
            num_scalar_prefetch=1,
            grid=(start,),
            in_specs=g_specs + specs + [pl.BlockSpec(memory_space=pl.ANY)] * len(so_far),
            out_specs=specs,
        ),
        out_shape=[jax.ShapeDtypeStruct(a.shape, a.dtype) for a in arrays],
        input_output_aliases={1 + len(flat) + 9 + i: i for i in range(len(so_far))},
        compiler_params=pltpu.CompilerParams(vmem_limit_bytes=60_000_000),
        cost_estimate=pl.CostEstimate(flops=600 * elements, bytes_accessed=22 * elements, transcendentals=elements),
        name="adam",
    )(me, *flat, *arrays, *so_far)


def solution(mesh):
    n = mesh.shape["dp"]
    ahead = [(i, (i + 1) % n) for i in range(n)]
    back = [(i, (i - 1) % n) for i in range(n)]

    def step(x, dy, *arrays):
        me = lax.axis_index("dp").astype(jnp.int32)[None]

        def place(*steps):
            return lambda s, me: (0, lax.rem(me + steps[0] + s * (steps[-1] - steps[0]), n))

        def everyone(s, me):
            return jnp.where(s < n, 1, 0), jnp.where(s < n, s, me)

        x, me = lax.optimization_barrier((x, me))
        summed, own = main_call(n, x, dy, *arrays[:3])
        half = own.shape[0] // 2
        from_left, from_right = lax.ppermute(own, "dp", ahead), lax.ppermute(own, "dp", back)
        new = adam_call(me, everyone, [summed, own], arrays)
        from_left, from_right, *new = lax.optimization_barrier((from_left, from_right, *new))
        top, bottom = lax.ppermute(from_left[:half], "dp", ahead), lax.ppermute(from_right[half:], "dp", back)
        new = adam_call(me, place(n - 1, n + 1), [from_left, from_right], arrays, new)
        return tuple(adam_call(me, place(2), [(top, bottom)], arrays, new))

    return jax.shard_map(
        step,
        mesh=mesh,
        in_specs=(P(("rep", "dp"), None, None),) * 2 + (P(None, None, None),) * 9,
        out_specs=(P("rep", None, None),) * 9,
        check_vma=False,
    )
```

```python
import functools

import jax
import jax.numpy as jnp
from jax import lax
from jax.experimental import pallas as pl
from jax.experimental.pallas import tpu as pltpu
from jax.sharding import PartitionSpec as P

BF16, F32 = jnp.bfloat16, jnp.float32
WIDE = 256
LANES = 128
TILE = 2048
FORWARD = 1024
ROWS = 512


def at(index, size):
    if isinstance(index, int):
        return pl.ds(index * size, size)
    return pl.ds(pl.multiple_of(index * size, size), size)


def dot(a, b):
    return jnp.dot(a, b, preferred_element_type=F32)


def dot_t(a, b):
    return lax.dot_general(a, b, (((1,), (1,)), ((), ())), preferred_element_type=F32)


def scale_of(wide):
    return lax.rsqrt(jnp.mean(wide * wide, -1, keepdims=True) + 1e-6)


def normed(h):
    wide = h.astype(F32)
    return (wide * scale_of(wide)).astype(BF16)


def main_kernel(
    n, x_hbm, dy_hbm, wg_hbm, wu_hbm, wd_hbm,
    all_hbm, own_hbm,
    h_ref, a_ref, at_ref, g_ref, gt_ref, da_ref, wgu_ref, wd_ref, hid_ref, dgu_ref, term_ref, one_ref, two_ref,
    w_sem, x_sem, dy_sem, one_send, one_recv, two_send, two_recv, near_send, near_recv, far_send, far_recv, keep_sem,
):
    tokens, d = h_ref.shape
    layers, ff, _ = wd_ref.shape
    full = ff // WIDE
    widths = [WIDE] * full + ([ff % WIDE] if ff % WIDE else [])
    share = d // n
    half = share // 2
    me = lax.axis_index("dp")
    right, left, across = (lax.rem(me + i, n) for i in (1, n - 1, 2))
    ways = (right, left)

    barrier = pltpu.get_barrier_semaphore()
    for way in ways:
        pl.semaphore_signal(barrier, inc=1, device_id={"dp": way}, device_id_type=pl.DeviceIdType.MESH)

    def cols_of(k):
        return pl.ds(pl.multiple_of(k * 3 * WIDE, 3 * WIDE), 3 * widths[k] if isinstance(k, int) else 3 * WIDE)

    def rows_of(owner, part=None):
        if part is None:
            return pl.ds(pl.multiple_of(owner * share, share), share)
        return pl.ds(pl.multiple_of(owner * share + part * half, half), half)

    def remote(source, target, send, recv, way):
        return pltpu.make_async_remote_copy(
            src_ref=source, dst_ref=target, send_sem=send, recv_sem=recv, device_id={"dp": ways[way]}, device_id_type=pl.DeviceIdType.MESH
        )

    def one(layer, k, way):
        cols = cols_of(k)
        return remote(term_ref.at[rows_of(across, way), cols], one_ref.at[way, :, cols], one_send.at[layer, k, way], one_recv.at[layer, k, way], way)

    def two(layer, k, way):
        cols = cols_of(k)
        return remote(term_ref.at[rows_of(ways[way]), cols], two_ref.at[way, :, cols], two_send.at[layer, k, way], two_recv.at[layer, k, way], way)

    def near(k, way):
        cols = cols_of(k)
        return remote(term_ref.at[rows_of(me), cols], all_hbm.at[rows_of(me), cols], near_send.at[k, way], near_recv.at[k, way], way)

    def far(k, way):
        cols = cols_of(k)
        block = all_hbm.at[rows_of(ways[1 - way], way), cols]
        return remote(block, block, far_send.at[k, way], far_recv.at[k, way], way)

    def keep(layer, k):
        cols = cols_of(k)
        target = all_hbm.at[rows_of(me), cols] if layer else own_hbm.at[:, cols]
        return pltpu.make_async_copy(term_ref.at[rows_of(me), cols], target, keep_sem.at[layer, k])

    def start_one(layer, k):
        for way in range(2):
            one(layer, k, way).start()

    def start_two(layer, k):
        cols = cols_of(k)
        for way in range(2):
            one(layer, k, way).wait()
            rows = rows_of(ways[way], way)
            term_ref[rows, cols] = (term_ref[rows, cols].astype(F32) + one_ref[way, :, cols].astype(F32)).astype(BF16)
        for way in range(2):
            two(layer, k, way).start()

    def finish(layer, k):
        cols = cols_of(k)
        rows = rows_of(me)
        for way in range(2):
            two(layer, k, way).wait()
        term_ref[rows, cols] = (term_ref[rows, cols].astype(F32) + two_ref[0, :, cols].astype(F32) + two_ref[1, :, cols].astype(F32)).astype(BF16)
        if layer:
            for way in range(2):
                near(k, way).start()
        keep(layer, k).start()

    def start_far(k):
        for way in range(2):
            near(k, way).wait()
        keep(1, k).wait()
        for way in range(2):
            far(k, way).start()

    def when(condition, action, *args):
        if isinstance(condition, bool):
            if condition:
                action(*args)
        else:
            pl.when(condition)(lambda: action(*args))

    def weight_copies(layer):
        copies = []
        for k, width in enumerate(widths):
            for source, offset in ((wg_hbm, 0), (wu_hbm, width)):
                copies.append((source.at[layer, :, pl.ds(k * WIDE, width)], wgu_ref.at[layer, :, pl.ds(2 * k * WIDE + offset, width)]))
        copies.append((wd_hbm.at[layer], wd_ref.at[layer]))
        return [pltpu.make_async_copy(source, target, w_sem.at[layer, i]) for i, (source, target) in enumerate(copies)]

    def x_copy(t, target):
        return pltpu.make_async_copy(x_hbm.at[0, at(t, ROWS)], target.at[at(t, ROWS)], x_sem.at[t])

    dy_copy = pltpu.make_async_copy(dy_hbm.at[0], g_ref, dy_sem)
    steps = tokens // ROWS
    for copy in weight_copies(0):
        copy.start()
    for t in range(steps):
        x_copy(t, h_ref).start()
    dy_copy.start()
    for layer in range(1, layers):
        for copy in weight_copies(layer):
            copy.start()
    for copy in weight_copies(0):
        copy.wait()

    def forward(t, carry):
        rows = at(t, FORWARD)
        for i in range(FORWARD // ROWS):
            x_copy(t * (FORWARD // ROWS) + i, h_ref).wait()
        x = h_ref[rows, :]
        a = normed(x)
        for k, width in enumerate(widths):
            gu = dot(a, wgu_ref[0, :, pl.ds(2 * k * WIDE, 2 * width)])
            gate, up = gu[:, :width], gu[:, width:]
            dgu_ref[pl.ds(k // 2 * FORWARD, FORWARD), pl.ds(k % 2 * WIDE, width)] = (gate * jax.nn.sigmoid(gate) * up).astype(BF16)
        down = 0.0
        for k in range(0, len(widths), 2):
            width = sum(widths[k : k + 2])
            down += dot(dgu_ref[pl.ds(k // 2 * FORWARD, FORWARD), pl.ds(0, width)], wd_ref[0, pl.ds(k * WIDE, width), :])
        h = (x.astype(F32) + down.astype(BF16).astype(F32)).astype(BF16)
        h_ref[rows, :] = h
        a = normed(h)
        a_ref[rows, :] = a
        at_ref[:, rows] = a.T
        return carry

    lax.fori_loop(0, tokens // FORWARD, forward, 0)
    dy_copy.wait()

    def turn(t, carry):
        rows = at(t, ROWS)
        gt_ref[:, rows] = g_ref[rows, :].T
        return carry

    lax.fori_loop(0, steps, turn, 0)
    for layer in range(1, layers):
        for copy in weight_copies(layer):
            copy.wait()

    def chunk(layer, k, width, first):
        gu_cols = pl.ds(pl.multiple_of(k * 2 * WIDE, 2 * WIDE), 2 * width)
        down_rows = pl.ds(pl.multiple_of(k * WIDE, WIDE), width)

        def hidden(t, carry):
            rows = at(t, TILE)
            gu = dot(a_ref[rows, :], wgu_ref[layer, :, gu_cols])
            dh = dot_t(g_ref[rows, :], wd_ref[layer, down_rows, :]).astype(BF16).astype(F32)
            gate, up = gu[:, :width], gu[:, width:]
            s = jax.nn.sigmoid(gate)
            silu = gate * s
            hid_ref[rows, pl.ds(0, width)] = (silu * up).astype(BF16)
            dgu_ref[rows, pl.ds(width, width)] = (dh * silu).astype(BF16)
            dgu_ref[rows, pl.ds(0, width)] = (dh * up * (s + silu * (1.0 - s))).astype(BF16)
            return carry

        lax.fori_loop(0, tokens // TILE, hidden, 0)
        if layer:
            when(k == 0, start_two, layer, last)
            when((k >= 1) & (k < full), start_two, layer, k - 1)

            @pl.when(k == full - 1)
            def _():
                for t in range(steps):
                    x_copy(t, a_ref).start()

        else:
            when(k >= 3, finish, layer, k - 3)
            when(k + 4 < full, start_far, k + 4)
        dgu = dot(at_ref[...], dgu_ref[:, pl.ds(0, 2 * width)]).astype(BF16)
        down = dot(gt_ref[...], hid_ref[:, pl.ds(0, width)]).astype(BF16)
        for j in range(width // LANES):
            for i, piece in enumerate((dgu[:, j * LANES : (j + 1) * LANES], dgu[:, width + j * LANES : width + (j + 1) * LANES], down[:, j * LANES : (j + 1) * LANES])):
                term_ref[:, pl.ds(pl.multiple_of(k * 3 * WIDE, 3 * WIDE) + (3 * j + i) * LANES, LANES)] = piece
        start_one(layer, k)
        if not layer:
            when(k >= 1, start_two, layer, k - 1)
        if layer:

            def by_a(t, carry):
                rows = at(t, TILE)
                part = dot_t(dgu_ref[rows, pl.ds(0, 2 * width)], wgu_ref[layer, :, gu_cols])
                if first:
                    da_ref[rows, :] = part
                else:
                    da_ref[rows, :] += part
                return carry

            lax.fori_loop(0, tokens // TILE, by_a, 0)
            when(k == 0, finish, layer, last)
            when(k == 1, finish, layer, 0)
            when(k == 2, start_far, last)
            when(k == 2, start_far, 0)
            when((k >= 3) & (k < full), finish, layer, k - 2)

    last = len(widths) - 1
    pl.semaphore_wait(barrier, 2)
    chunk(1, last, widths[last], True)
    lax.fori_loop(0, full, lambda k, carry: (chunk(1, k, WIDE, False), carry)[1], 0)


    def between(t, carry):
        rows = at(t, ROWS)
        x_copy(t, a_ref).wait()
        da = da_ref[rows, :].astype(BF16).astype(F32)
        h = h_ref[rows, :].astype(F32)
        r = scale_of(h)
        inner = jnp.mean(da * h, -1, keepdims=True)
        dh = (r * (da - h * (r * r * inner))).astype(BF16).astype(F32)
        g = (g_ref[rows, :].astype(F32) + dh).astype(BF16)
        g_ref[rows, :] = g
        gt_ref[:, rows] = g.T
        a = normed(a_ref[rows, :])
        a_ref[rows, :] = a
        at_ref[:, rows] = a.T
        return carry

    lax.fori_loop(0, steps // 4, between, 0)
    start_two(1, full - 1)
    finish(1, full - 2)
    start_far(1)
    start_far(2)
    lax.fori_loop(steps // 4, steps, between, 0)
    finish(1, full - 1)
    start_far(3)
    lax.fori_loop(0, full, lambda k, carry: (chunk(0, k, WIDE, False), carry)[1], 0)
    chunk(0, last, widths[last], False)
    finish(0, last - 2)
    start_two(0, last)
    finish(0, last - 1)
    finish(0, last)
    for k in range(len(widths)):
        keep(0, k).wait()
        for way in range(2):
            far(k, way).wait()


def main_call(n, x, dy, wg, wu, wd):
    layers, d, ff = wg.shape
    tokens = x.shape[1]
    if layers != 2 or n != 4:
        raise ValueError("unsupported sizes")
    chunks = -(-ff // WIDE)
    any_ = pl.BlockSpec(memory_space=pl.ANY)
    share = d // n
    sems = pltpu.SemaphoreType.DMA
    return pl.pallas_call(
        functools.partial(main_kernel, n),
        out_shape=[jax.ShapeDtypeStruct((d, 3 * ff), BF16), jax.ShapeDtypeStruct((share, 3 * ff), BF16)],
        in_specs=[any_] * 5,
        out_specs=[any_] * 2,
        scratch_shapes=[
            pltpu.VMEM((tokens, d), BF16),
            pltpu.VMEM((tokens, d), BF16),
            pltpu.VMEM((d, tokens), BF16),
            pltpu.VMEM((tokens, d), BF16),
            pltpu.VMEM((d, tokens), BF16),
            pltpu.VMEM((tokens, d), F32),
            pltpu.VMEM((layers, d, 2 * ff), BF16),
            pltpu.VMEM((layers, ff, d), BF16),
            pltpu.VMEM((tokens, WIDE), BF16),
            pltpu.VMEM((tokens, 2 * WIDE), BF16),
            pltpu.VMEM((d, 3 * ff), BF16),
            pltpu.VMEM((2, share // 2, 3 * ff), BF16),
            pltpu.VMEM((2, share, 3 * ff), BF16),
            sems((layers, 2 * chunks + 1)),
            sems((tokens // ROWS,)),
            sems,
            *[sems((layers, chunks, 2))] * 4,
            *[sems((chunks, 2))] * 4,
            sems((layers, chunks)),
        ],
        compiler_params=pltpu.CompilerParams(vmem_limit_bytes=67_000_000, collective_id=0, has_side_effects=True),
        name="main",
    )(x, dy, wg, wu, wd)


def adamw(w, m, v, g):
    m = 0.9 * m + 0.1 * g
    v = 0.95 * v + 0.05 * g * g
    step = m * lax.rsqrt(v + 1e-8) + 0.1 * w
    return (w - 0.02 * step).astype(BF16), m, v


def adam_kernel(sources, me, *refs):
    count = sum(parts for _, parts in sources)
    ins, outs = refs[count : count + 9], refs[-9:]
    units = ins[0].shape[-1]
    start = 0
    for steps, parts in sources:
        mine, refs = refs[:parts], refs[parts:]

        @pl.when((pl.program_id(0) >= start) & (pl.program_id(0) < start + steps))
        def _(mine=mine):
            def unit(j, carry, mine=mine):
                cols = at(j, LANES)
                for i in range(3):
                    g = [ref[:, at(3 * j + i, LANES)].astype(F32) for ref in mine]
                    g = jnp.concatenate(g, 0) if len(g) > 1 else g[0]
                    index = (0, slice(None), cols)
                    if i == 2:
                        g, index = g.T, (0, cols, slice(None))
                    w, m, v = adamw(ins[i][index].astype(F32), ins[3 + i][index], ins[6 + i][index], g)
                    outs[i][index], outs[3 + i][index], outs[6 + i][index] = w, m, v
                return carry

            if len(sources) == 1:
                for j in range(units // LANES):
                    unit(j, 0)
            else:
                lax.fori_loop(0, units // LANES, unit, 0)

        start += steps


def adam_call(me, places, sources, arrays, so_far=()):
    layers, d, ff = arrays[0].shape
    sources = [source if isinstance(source, tuple) else (source,) for source in sources]

    def at_row(s, me):
        layer, place = places(s, me[0])
        return layer, place, 0

    def at_column(s, me):
        layer, place = places(s, me[0])
        return layer, 0, place

    row, column = pl.BlockSpec((1, LANES, ff), at_row), pl.BlockSpec((1, ff, LANES), at_column)
    specs = [row, row, column] * 3
    flat, g_specs, steps, start = [], [], [], 0
    for source in sources:
        size = LANES // len(source)
        blocks = source[0].shape[0] // size
        for array in source:
            flat.append(array)
            g_specs.append(pl.BlockSpec((size, 3 * ff), lambda s, me, start=start, blocks=blocks: (jnp.clip(s - start, 0, blocks - 1), 0)))
        steps.append((blocks, len(source)))
        start += blocks
    elements = start * 3 * LANES * ff
    return pl.pallas_call(
        functools.partial(adam_kernel, steps),
        grid_spec=pltpu.PrefetchScalarGridSpec(
            num_scalar_prefetch=1,
            grid=(start,),
            in_specs=g_specs + specs + [pl.BlockSpec(memory_space=pl.ANY)] * len(so_far),
            out_specs=specs,
        ),
        out_shape=[jax.ShapeDtypeStruct(a.shape, a.dtype) for a in arrays],
        input_output_aliases={1 + len(flat) + 9 + i: i for i in range(len(so_far))},
        compiler_params=pltpu.CompilerParams(vmem_limit_bytes=60_000_000),
        cost_estimate=pl.CostEstimate(flops=600 * elements, bytes_accessed=22 * elements, transcendentals=elements),
        name="adam",
    )(me, *flat, *arrays, *so_far)


def solution(mesh):
    n = mesh.shape["dp"]
    ahead = [(i, (i + 1) % n) for i in range(n)]
    back = [(i, (i - 1) % n) for i in range(n)]

    def step(x, dy, *arrays):
        me = lax.axis_index("dp").astype(jnp.int32)[None]

        def place(*steps):
            return lambda s, me: (0, lax.rem(me + steps[0] + s * (steps[-1] - steps[0]), n))

        def everyone(s, me):
            return jnp.where(s < n, 1, 0), jnp.where(s < n, s, me)

        x, me = lax.optimization_barrier((x, me))
        summed, own = main_call(n, x, dy, *arrays[:3])
        half = own.shape[0] // 2
        from_left, from_right = lax.ppermute(own, "dp", ahead), lax.ppermute(own, "dp", back)
        new = adam_call(me, everyone, [summed, own], arrays)
        from_left, from_right, *new = lax.optimization_barrier((from_left, from_right, *new))
        top, bottom = lax.ppermute(from_left[:half], "dp", ahead), lax.ppermute(from_right[half:], "dp", back)
        new = adam_call(me, place(n - 1, n + 1), [from_left, from_right], arrays, new)
        return tuple(adam_call(me, place(2), [(top, bottom)], arrays, new))

    return jax.shard_map(
        step,
        mesh=mesh,
        in_specs=(P(("rep", "dp"), None, None),) * 2 + (P(None, None, None),) * 9,
        out_specs=(P("rep", None, None),) * 9,
        check_vma=False,
    )
```
